256 devices in a mesh: gx: 16 (over y, x), gy: 16 (over z, core).
Axes of the slice: x: 4, y: 4, z: 8, core: 2. Of those that a mesh axis runs over, the one named last changes fastest.
Arguments:
- source_heat: float32 [160, 256, 2048], P(None, 'gx', 'gy'), may hold values from -8 to 8
- horiz_coef: float32 [160], replicated, may hold values from 0.5 to 4
- face_coef: float32 [161], replicated, may hold values from 0.25 to 4
- column_inverse: float32 [160, 160], replicated, as said below
Outputs:
- pressure: float32 [160, 256, 2048], P(None, 'gx', 'gy')
- true_residual: float32 [160, 256, 2048], P(None, 'gx', 'gy')
The draws below stay inside these ranges and needn't reach their ends.
Inputs may be any that keep to these rules, and one draw needn't show every extreme that they name: `column_inverse`: the inverse of the tridiagonal matrix with diagonal 4 horiz_coef[k] + face_coef[k] + face_coef[k+1] and off-diagonal entries -face_coef[k] between levels k-1 and k.
All inputs are finite; a program needn't handle non-finite values.
Results may differ from the reference program's by a relative error of at most 0.0003.
Values sent between devices are 32-bit elements; how exact they have to be, the bound alone decides.
No kernel may reach another device: no remote copies, remote signals or barrier semaphores. Data moves between devices by JAX's collectives and lax.ppermute only.
A program may use at most 64 MiB of HBM per device.

```python
import jax
import jax.numpy as jnp
from jax import lax

NZ = 160
ITERS = 3
NX = 256
NY = 2048


def column_setup(key):
    base = jax.random.fold_in(key, 11)
    key_horiz = jax.random.fold_in(base, 1)
    key_faces = jax.random.fold_in(base, 2)
    horizontal = jnp.exp(jax.random.uniform(key_horiz, (NZ,), jnp.float32, jnp.log(0.5), jnp.log(4.0)))
    face_coef = jnp.exp(jax.random.uniform(key_faces, (NZ + 1,), jnp.float32, jnp.log(0.25), jnp.log(4.0)))
    diagonal = 4.0 * horizontal + face_coef[:-1] + face_coef[1:]
    tridiag = jnp.diag(diagonal) - jnp.diag(face_coef[1:-1], 1) - jnp.diag(face_coef[1:-1], -1)
    inverse = jnp.linalg.solve(tridiag, jnp.eye(NZ, dtype=jnp.float32))
    return (horizontal, face_coef, inverse)


def draw_horiz_coef(key, part):
    return column_setup(key)[0]


def draw_face_coef(key, part):
    return column_setup(key)[1]


def draw_column_inverse(key, part):
    return column_setup(key)[2]


def draw_source_heat(key, part):
    noise_key = jax.random.fold_in(key, 23)
    return jnp.clip(jax.random.normal(noise_key, (NZ, NX, NY), jnp.float32), -8.0, 8.0)


def setup_inputs(seed: int = 0) -> dict:
    streams_of = jax.random.split(jax.random.key(seed), 5)
    return {
        "source_heat": draw_source_heat(jax.random.fold_in(streams_of[4], 71), 0),
        "horiz_coef": draw_horiz_coef(jax.random.fold_in(streams_of[4], 71), 0),
        "face_coef": draw_face_coef(jax.random.fold_in(streams_of[4], 71), 0),
        "column_inverse": draw_column_inverse(jax.random.fold_in(streams_of[4], 71), 0),
    }


def operate(values_in, horizontal, face_coef):
    padded = jnp.pad(values_in, ((0, 0), (1, 1), (1, 1)), mode='wrap')
    beside = padded[:, 2:, 1:-1] + padded[:, :-2, 1:-1] + padded[:, 1:-1, 2:] + padded[:, 1:-1, :-2]
    zero_layer = jnp.zeros_like(values_in[:1])
    upward = jnp.concatenate([values_in[1:], zero_layer], 0)
    downward = jnp.concatenate([zero_layer, values_in[:-1]], 0)
    lower_face = face_coef[:-1][:, None, None]
    upper_face = face_coef[1:][:, None, None]
    return horizontal[:, None, None] * (4.0 * values_in - beside) + upper_face * (values_in - upward) + lower_face * (values_in - downward)

def precondition(values_in, column_inverse):
    layout = values_in.shape
    columns = values_in.reshape(layout[0], -1)
    return jnp.dot(column_inverse, columns, precision=lax.Precision.HIGHEST).reshape(layout)

def reference(source_heat, horiz_coef, face_coef, column_inverse):
    pressure = jnp.zeros_like(source_heat)
    residual = source_heat
    precond = precondition(residual, column_inverse)
    direction = precond
    inner = jnp.sum(residual * precond)
    for iteration in range(ITERS):
        image = operate(direction, horiz_coef, face_coef)
        step_len = inner / jnp.sum(direction * image)
        pressure = pressure + step_len * direction
        residual = residual - step_len * image
        if iteration + 1 < ITERS:
            precond = precondition(residual, column_inverse)
            inner_next = jnp.sum(residual * precond)
            direction = precond + inner_next / inner * direction
            inner = inner_next
    true_residual = source_heat - operate(pressure, horiz_coef, face_coef)
    return (pressure, true_residual)
```

```python
import jax
import jax.numpy as jnp
from jax import lax
from jax.experimental import pallas as pl
from jax.experimental.pallas import tpu as pltpu
from jax.sharding import Mesh
from jax.sharding import PartitionSpec as P

F32 = jnp.float32
LANES = 128
EDGE = 6
STEPS = 3


def vmem(rows, cols=LANES):
    return pltpu.VMEM((rows, cols), F32)


def spec():
    return pl.BlockSpec(memory_space=pltpu.VMEM)


def params(mib):
    return pltpu.CompilerParams(vmem_limit_bytes=mib * 1024 * 1024)


def cost(flops, size):
    return pl.CostEstimate(flops=flops, bytes_accessed=size, transcendentals=0)


def lane_ids(rows):
    return lax.broadcasted_iota(jnp.int32, (rows, LANES), 1)


def product(matrix, columns):
    return jnp.dot(matrix, columns, precision=lax.Precision.HIGHEST, preferred_element_type=F32)


def apply_inverse(matrix, src, dst, nz, tiles, width):
    def some(first, count):
        parts = [src[pl.ds(pl.multiple_of((first + t) * nz, 8), nz), :] for t in range(count)]
        out = product(matrix, jnp.concatenate(parts, axis=1) if count > 1 else parts[0])
        for t in range(count):
            dst[pl.ds(pl.multiple_of((first + t) * nz, 8), nz), :] = out[:, t * LANES : (t + 1) * LANES]

    whole = tiles // width

    def body(i, carry):
        some(i * width, width)
        return carry

    lax.fori_loop(0, whole, body, 0)
    if tiles % width:
        some(whole * width, tiles % width)


def load_kernel(nz, nx, b_hbm, nat, low, high, sem):
    copy = pltpu.make_async_copy(b_hbm, nat, sem)
    copy.start()
    copy.wait()
    for i in range(STEPS):
        low[i * nz : (i + 1) * nz, :] = nat[pl.ds(i, nz, stride=nx), :]
        high[i * nz : (i + 1) * nz, :] = nat[pl.ds(nx - STEPS + i, nz, stride=nx), :]


def own_kernel(nz, nx, nat, h_row, inv, b_t, u0, h_wide, edge):
    eye = lax.broadcasted_iota(jnp.int32, (nz, nz), 0) == lax.broadcasted_iota(jnp.int32, (nz, nz), 1)
    column = jnp.sum(jnp.where(eye, jnp.broadcast_to(h_row[...], (nz, nz)), 0.0), axis=1, keepdims=True)
    h_wide[...] = jnp.broadcast_to(column, (nz, LANES))
    lane = lane_ids(nz)
    packed = jnp.zeros((nz, LANES), F32)
    for x in range(nx):
        row = nat[pl.ds(x, nz, stride=nx), :]
        b_t[x * nz : (x + 1) * nz, :] = row
        at = EDGE * (x + 2)
        packed = jnp.where((lane >= at) & (lane < at + EDGE), pltpu.roll(row, at + 3, 1), packed)
    edge[...] = packed
    apply_inverse(inv[...], b_t, u0, nz, nx, 4)


def pack_kernel(nz, nx, edge, below, above, packed):
    lane = lane_ids(nz)
    out = edge[...]
    for x, ref, i in ((-2, below, 1), (-1, below, 2), (nx, above, 0), (nx + 1, above, 1)):
        at = EDGE * (x + 2)
        row = ref[i * nz : (i + 1) * nz, :]
        out = jnp.where((lane >= at) & (lane < at + EDGE), pltpu.roll(row, (at + 3) % LANES, 1), out)
    packed[...] = out


def outer_kernel(nz, nx, u0, below, above, inv, u0e):
    u0e[STEPS * nz : (STEPS + nx) * nz, :] = u0[...]
    for ref, first in ((below, 0), (above, STEPS + nx)):
        out = product(inv[...], jnp.concatenate([ref[i * nz : (i + 1) * nz, :] for i in range(STEPS)], axis=1))
        for i in range(STEPS):
            u0e[(first + i) * nz : (first + i + 1) * nz, :] = out[:, i * LANES : (i + 1) * LANES]


def stencil_row(v, top, here, nz, x, side, lane):
    row = lambda r: v[pl.ds(pl.multiple_of(r * nz, 8), nz), :]
    mid = row(here)
    turned = pltpu.roll(side, lax.rem(2 * LANES - (EDGE * (x + 2) + 3), LANES), 1)
    left = jnp.where(lane == 0, turned, pltpu.roll(mid, 1, 1))
    right = jnp.where(lane == LANES - 1, turned, pltpu.roll(mid, LANES - 1, 1))
    return row(here - 1) + row(here + 1) + left + right, mid


def pack_row(packed, mid, x, lane):
    at = EDGE * (x + 2)
    turned = pltpu.roll(mid, lax.rem(at + 3, LANES), 1)
    return jnp.where((lane == at + 2) | (lane == at + 3), turned, packed)


def stencil(v, base, g, side_ref, h_ref, nz, first, count, pack_first, pack_count, side_out):
    lane = lane_ids(nz)

    def body(i, packed):
        x = first + i
        around, mid = stencil_row(v, None, x - base, nz, x, side_ref[...], lane)
        g[pl.ds(pl.multiple_of(i * nz, 8), nz), :] = h_ref[...] * around
        return pack_row(packed, mid, x, lane)

    packed = lax.fori_loop(0, count, body, jnp.zeros((nz, LANES), F32))
    if side_out is not None:
        side = side_ref[...]
        pos = lax.rem(lane, EDGE)
        after = jnp.where(pos == 2, packed, pltpu.roll(side, LANES - 1, 1))
        before = jnp.where(pos == 3, packed, pltpu.roll(side, 1, 1))
        rows = pltpu.roll(side, EDGE, 1) + pltpu.roll(side, LANES - EDGE, 1)
        side_out[...] = h_ref[...] * (after + before + rows)


def fold(v):
    out = v[0:8]
    for i in range(1, v.shape[0] // 8):
        out = out + v[8 * i : 8 * i + 8]
    return out


def krylov_kernel(nz, nx, members, b_t, u0e, from_left, from_right, inv, h_wide, u1e, u2e, g1e, g2e, g3, send, side):
    lane = lane_ids(nz)
    pos = lax.rem(lane, EDGE)
    near = jnp.where(pos < 3, from_left[...], from_right[...])
    turned = jnp.zeros_like(near)
    for p in range(EDGE):
        turned = jnp.where(pos == p, pltpu.roll(near, (LANES - (5 - 2 * p)) % LANES, 1), turned)
    side[...] = product(inv[...], turned)
    n1 = nx + 4
    stencil(u0e, -3, g1e, side, h_wide, nz, -2, n1, -1, nx + 2, g1e.at[pl.ds(n1 * nz, nz), :])
    apply_inverse(inv[...], g1e, u1e, nz, n1 + 1, 4)
    n2 = nx + 2
    side[...] = u1e[n1 * nz : (n1 + 1) * nz, :]
    stencil(u1e, -2, g2e, side, h_wide, nz, -1, n2, 0, nx, g2e.at[pl.ds(n2 * nz, nz), :])
    apply_inverse(inv[...], g2e, u2e, nz, n2 + 1, 4)
    side[...] = u2e[n2 * nz : (n2 + 1) * nz, :]

    def body(x, sums):
        at = lambda ref, r: ref[pl.ds(pl.multiple_of(r * nz, 8), nz), :]
        around, w2 = stencil_row(u2e, None, x + 1, nz, x, side[...], lane)
        next_g = h_wide[...] * around
        g3[pl.ds(pl.multiple_of(x * nz, 8), nz), :] = next_g
        b, f1, f2 = at(b_t, x), at(g1e, x + 2), at(g2e, x + 1)
        v0, v1 = at(u0e, x + 3), at(u1e, x + 2)
        a0, a1, a2 = b - f1, f1 - f2, f2 - next_g
        terms = (v0 * a0, v1 * a0, v1 * a1, w2 * a0, w2 * a1, w2 * a2, v0 * b, v1 * b, w2 * b)
        return tuple(s + fold(t) for s, t in zip(sums, terms))

    zero = jnp.zeros((8, LANES), F32)
    sums = lax.fori_loop(0, nx, body, (zero,) * 9)
    line = lax.broadcasted_iota(jnp.int32, (8, LANES), 1)
    out = zero
    for i, s in enumerate(sums):
        total = jnp.sum(jnp.sum(s, axis=0, keepdims=True), axis=1, keepdims=True)
        out = jnp.where(line == i, jnp.broadcast_to(total, (8, LANES)), out)
    for i in range(members // 8):
        send[8 * i : 8 * i + 8, :] = out


def solve_small(t):
    g00, g10, g11, g20, g21, g22, m0, m1, m2 = t
    l1, l2 = g10 / g00, g20 / g00
    d1 = g11 - l1 * g10
    e = g21 - l2 * g10
    l3 = e / d1
    d2 = g22 - l2 * g20 - l3 * e
    y1 = m1 - l1 * m0
    y2 = m2 - l2 * m0 - l3 * y1
    c2 = y2 / d2
    c1 = y1 / d1 - l3 * c2
    return m0 / g00 - l1 * c1 - l2 * c2, c1, c2


def combine_kernel(nz, nx, kz, got, b_t, u0e, u1e, u2e, g1e, g2e, g3, pressure, true_residual, coef):
    step = pl.program_id(0)

    @pl.when(step == 0)
    def _():
        total = jnp.sum(fold(got[...]), axis=0, keepdims=True)
        line = lax.broadcasted_iota(jnp.int32, (1, LANES), 1)
        pick = lambda i: jnp.sum(jnp.where(line == i, total, 0.0), axis=1, keepdims=True)
        for i, c in enumerate(solve_small([pick(i) for i in range(9)])):
            coef[i * 8 : i * 8 + 8, :] = jnp.broadcast_to(c, (8, LANES))

    c0, c1, c2 = (jnp.concatenate([coef[i * 8 : i * 8 + 8, :]] * (kz // 8), axis=0) for i in range(3))

    def body(x, carry):
        at = lambda ref, r: ref[pl.ds(pl.multiple_of(r * nz + step * kz, 8), kz), :]
        v0, v1, v2 = at(u0e, x + 3), at(u1e, x + 2), at(u2e, x + 1)
        b, f1, f2, f3 = at(b_t, x), at(g1e, x + 2), at(g2e, x + 1), at(g3, x)
        pressure[pl.ds(x, kz, stride=nx), :] = c0 * v0 + c1 * v1 + c2 * v2
        true_residual[pl.ds(x, kz, stride=nx), :] = b - (c0 * (b - f1) + c1 * (f1 - f2) + c2 * (f2 - f3))
        return carry

    lax.fori_loop(0, nx, body, 0)


def neighbours(array, axes, up):
    size = lax.axis_size(axes)
    pairs = [(i, (i + 1) % size) for i in range(size)]
    return lax.ppermute(array, axes, pairs if up else [(b, a) for a, b in pairs])


def on_device(source_heat, horiz_coef, face_coef, column_inverse):
    nz, nx, ny = source_heat.shape
    gx, gy = "gx", "gy"
    members = lax.axis_size(gx) * lax.axis_size(gy)
    part = lambda f, *a: (lambda *refs: f(*a, *refs))
    nat, low, high = pl.pallas_call(
        part(load_kernel, nz, nx),
        in_specs=[pl.BlockSpec(memory_space=pltpu.HBM)],
        out_specs=[spec()] * 3,
        out_shape=[vmem(nz * nx), vmem(STEPS * nz), vmem(STEPS * nz)],
        scratch_shapes=[pltpu.SemaphoreType.DMA],
        compiler_params=params(4),
    )(source_heat.reshape(nz * nx, ny))
    below = neighbours(high, gx, True)
    above = neighbours(low, gx, False)
    b_t, u0, h_wide, edge = pl.pallas_call(
        part(own_kernel, nz, nx),
        in_specs=[spec()] * 3,
        out_specs=[spec()] * 4,
        out_shape=[vmem(nz * nx), vmem(nz * nx), vmem(nz), vmem(nz)],
        compiler_params=params(8),
        cost_estimate=cost(12 * nz * nz * nx * ny, 1 << 20),
    )(nat, horiz_coef.reshape(1, nz), column_inverse)
    packed = pl.pallas_call(
        part(pack_kernel, nz, nx),
        in_specs=[spec()] * 3,
        out_specs=spec(),
        out_shape=vmem(nz),
        compiler_params=params(4),
    )(edge, below, above)
    from_left = neighbours(packed, gy, True)
    from_right = neighbours(packed, gy, False)
    u0e = pl.pallas_call(
        part(outer_kernel, nz, nx),
        in_specs=[spec()] * 4,
        out_specs=spec(),
        out_shape=vmem((nx + 6) * nz),
        compiler_params=params(8),
        cost_estimate=cost(12 * nz * nz * 6 * ny, 1 << 20),
    )(u0, below, above, column_inverse)
    u1e, u2e, g1e, g2e, g3, send = pl.pallas_call(
        part(krylov_kernel, nz, nx, members),
        in_specs=[spec()] * 6,
        out_specs=[spec()] * 6,
        out_shape=[
            vmem((nx + 5) * nz),
            vmem((nx + 3) * nz),
            vmem((nx + 5) * nz),
            vmem((nx + 3) * nz),
            vmem(nx * nz),
            vmem(members),
        ],
        scratch_shapes=[pltpu.VMEM((nz, LANES), F32)],
        compiler_params=params(8),
        cost_estimate=cost(36 * nz * nz * nx * ny, 1 << 20),
    )(b_t, u0e, from_left, from_right, column_inverse, h_wide)
    got = lax.all_to_all(send.reshape(members, 1, LANES), (gx, gy), split_axis=0, concat_axis=0, tiled=True)
    kz = 32
    pressure, true_residual = pl.pallas_call(
        part(combine_kernel, nz, nx, kz),
        grid=(nz // kz,),
        in_specs=[spec()] * 8,
        out_specs=[pl.BlockSpec((kz * nx, ny), lambda i: (i, 0))] * 2,
        out_shape=[jax.ShapeDtypeStruct((nz * nx, ny), F32)] * 2,
        scratch_shapes=[pltpu.VMEM((24, LANES), F32)],
        compiler_params=params(8),
    )(got.reshape(members, LANES), b_t, u0e, u1e, u2e, g1e, g2e, g3)
    return pressure.reshape(nz, nx, ny), true_residual.reshape(nz, nx, ny)


def solution(mesh):
    field = P(None, "gx", "gy")
    return jax.shard_map(
        on_device,
        mesh=mesh,
        in_specs=(field, P(), P(), P()),
        out_specs=(field, field),
        check_vma=False,
    )
```

```python
import jax
import jax.numpy as jnp
from jax import lax
from jax.experimental import pallas as pl
from jax.experimental.pallas import tpu as pltpu
from jax.sharding import Mesh
from jax.sharding import PartitionSpec as P

F32 = jnp.float32
LANES = 128
GROUP = 9
STEPS = 3


def vmem(rows, cols=LANES):
    return pltpu.VMEM((rows, cols), F32)


def spec():
    return pl.BlockSpec(memory_space=pltpu.VMEM)


def params(mib):
    return pltpu.CompilerParams(vmem_limit_bytes=mib * 1024 * 1024)


def cost(flops, size):
    return pl.CostEstimate(flops=flops, bytes_accessed=size, transcendentals=0)


def lane_ids(rows):
    return lax.broadcasted_iota(jnp.int32, (rows, LANES), 1)


def product(matrix, columns):
    return jnp.dot(matrix, columns, precision=lax.Precision.HIGHEST, preferred_element_type=F32)


def apply_inverse(matrix, src, dst, nz, tiles, width):
    def some(first, count):
        parts = [src[pl.ds(pl.multiple_of((first + t) * nz, 8), nz), :] for t in range(count)]
        out = product(matrix, jnp.concatenate(parts, axis=1) if count > 1 else parts[0])
        for t in range(count):
            dst[pl.ds(pl.multiple_of((first + t) * nz, 8), nz), :] = out[:, t * LANES : (t + 1) * LANES]

    whole = tiles // width

    def body(i, carry):
        some(i * width, width)
        return carry

    lax.fori_loop(0, whole, body, 0)
    if tiles % width:
        some(whole * width, tiles % width)


def load_kernel(nz, nx, nat, low, high):
    for i in range(STEPS):
        low[i * nz : (i + 1) * nz, :] = nat[pl.ds(i, nz, stride=nx), :]
        high[i * nz : (i + 1) * nz, :] = nat[pl.ds(nx - STEPS + i, nz, stride=nx), :]


def strip_places(nx):
    half = nx // 2
    count = half + 2 * STEPS
    return [(t, t * half - STEPS + r, r) for t in range(2) for r in range(count)]


def add_edges(row, group, lane, inner, outer):
    first = GROUP * group
    turned = pltpu.roll(row, (first + STEPS) % LANES, 1)
    shifted = lax.rem(lane + (LANES - first), LANES)
    inner = jnp.where(shifted < GROUP, turned, inner)
    outer = jnp.where(lax.rem(shifted + STEPS, LANES) < GROUP, turned, outer)
    return inner, outer


def pack_edges(rows, first_x, nx, nz, inner, outer, tile, fresh):
    lane = lane_ids(tile)
    wanted, have = rows

    def body(i, carry):
        k = i * tile
        for t in range(2):
            at = pl.ds(pl.multiple_of(t * nz + k, 8), tile)
            if fresh:
                packed = (jnp.zeros((tile, LANES), F32),) * 2
            else:
                packed = (inner[at, :], outer[at, :])
            for u, x, group in strip_places(nx):
                if u == t and x in wanted:
                    packed = add_edges(have(x, k), group, lane, *packed)
            inner[at, :], outer[at, :] = packed
        return carry

    lax.fori_loop(0, nz // tile, body, 0, unroll=2)


def own_kernel(nz, nx, nat, h_row, inv, b_t, u0, h_wide, inner, outer):
    eye = lax.broadcasted_iota(jnp.int32, (nz, nz), 0) == lax.broadcasted_iota(jnp.int32, (nz, nz), 1)
    column = jnp.sum(jnp.where(eye, jnp.broadcast_to(h_row[...], (nz, nz)), 0.0), axis=1, keepdims=True)
    h_wide[...] = jnp.broadcast_to(column, (nz, LANES))
    for x in range(nx):
        b_t[x * nz : (x + 1) * nz, :] = nat[pl.ds(x, nz, stride=nx), :]
    have = lambda x, k: b_t[pl.ds(pl.multiple_of(x * nz + k, 8), 8), :]
    pack_edges((range(nx), have), 0, nx, nz, inner, outer, 8, True)
    apply_inverse(inv[...], b_t, u0, nz, nx, nx)


def pack_kernel(nz, nx, inner_own, outer_own, below, above, inner, outer):
    inner[...] = inner_own[...]
    outer[...] = outer_own[...]

    def have(x, k):
        ref, r = (below, x + STEPS) if x < 0 else (above, x - nx)
        return ref[pl.ds(pl.multiple_of(r * nz + k, 8), 8), :]

    wanted = [*range(-STEPS, 0), *range(nx, nx + STEPS)]
    pack_edges((wanted, have), -STEPS, nx, nz, inner, outer, 8, False)


def rows_at(ref, k, tile, nz):
    return lambda r: ref[pl.ds(pl.multiple_of(r * nz + k, 8), tile), :]


def sideways(mid, step=1):
    return pltpu.roll(mid, step, 1) + pltpu.roll(mid, LANES - step, 1)


def stencil(v, g, h_ref, nz, count, tile=8, unroll=4):
    def body(i, carry):
        k = i * tile
        load = rows_at(v, k, tile, nz)
        h = h_ref[pl.ds(pl.multiple_of(k, 8), tile), :]
        for j in range(count):
            g[pl.ds(pl.multiple_of(j * nz + k, 8), tile), :] = h * ((load(j) + load(j + 2)) + sideways(load(j + 1)))
        return carry

    lax.fori_loop(0, nz // tile, body, 0, unroll=unroll)


def inner_terms(b, f1, f2, f3, v0, v1, v2):
    a0, a1, a2 = b - f1, f1 - f2, f2 - f3
    return v0 * a0, v1 * a0, v1 * a1, v2 * a0, v2 * a1, v2 * a2, v0 * b, v1 * b, v2 * b


def add_all(a, b):
    return tuple(p + q for p, q in zip(a, b))


def main_kernel(nz, nx, b_t, u0, below, above, inv, h_wide, u0e, u1e, u2e, g1e, g2e, g3, sums_out):
    u0e[STEPS * nz : (STEPS + nx) * nz, :] = u0[...]
    for ref, first in ((below, 0), (above, STEPS + nx)):
        out = product(inv[...], jnp.concatenate([ref[i * nz : (i + 1) * nz, :] for i in range(STEPS)], axis=1))
        for i in range(STEPS):
            u0e[(first + i) * nz : (first + i + 1) * nz, :] = out[:, i * LANES : (i + 1) * LANES]
    stencil(u0e, g1e, h_wide, nz, nx + 4)
    apply_inverse(inv[...], g1e, u1e, nz, nx + 4, nx + 4)
    stencil(u1e, g2e, h_wide, nz, nx + 2)
    apply_inverse(inv[...], g2e, u2e, nz, nx + 2, nx + 2)
    tile = 8

    def body(i, sums):
        k = i * tile
        at_b, at_0, at_1, at_2, at_f1, at_f2 = (rows_at(ref, k, tile, nz) for ref in (b_t, u0e, u1e, u2e, g1e, g2e))
        h = h_wide[pl.ds(pl.multiple_of(k, 8), tile), :]
        part = None
        for x in range(nx):
            v2 = at_2(x + 1)
            f3 = h * ((at_2(x) + at_2(x + 2)) + sideways(v2))
            g3[pl.ds(pl.multiple_of(x * nz + k, 8), tile), :] = f3
            terms = inner_terms(at_b(x), at_f1(x + 2), at_f2(x + 1), f3, at_0(x + 3), at_1(x + 2), v2)
            part = terms if part is None else add_all(part, terms)
        return add_all(sums, part)

    sums = lax.fori_loop(0, nz // tile, body, (jnp.zeros((tile, LANES), F32),) * 9)
    lane = lane_ids(tile)
    for i, s in enumerate(sums):
        sums_out[8 * i : 8 * i + 8, :] = jnp.where((lane >= STEPS) & (lane < LANES - STEPS), s, 0.0)


def strip_kernel(nz, nx, members, inner, outer, left, right, inv, h_wide, sums_in, bs, u0s, u1s, u2s, g1s, g2s, g3s, send):
    tile = 8
    lane = lane_ids(nz)
    pos = lax.rem(lane, GROUP)
    used = lane < GROUP * (nx // 2 + 2 * STEPS)
    for t in range(2):
        at = slice(t * nz, (t + 1) * nz)
        bs[t * nz : (t + 1) * nz, :] = jnp.where((pos < STEPS) & used, left[at, :], inner[at, :])
        bs[(t + 2) * nz : (t + 3) * nz, :] = jnp.where((pos >= STEPS) & (pos < 2 * STEPS) & used, right[at, :], outer[at, :])

    def spread(v, g):
        def body(i, carry):
            k = i * tile
            load = rows_at(v, k, tile, nz)
            h = h_wide[pl.ds(pl.multiple_of(k, 8), tile), :]
            for j in range(4):
                mid = load(j)
                g[pl.ds(pl.multiple_of(j * nz + k, 8), tile), :] = h * (sideways(mid) + sideways(mid, GROUP))
            return carry

        lax.fori_loop(0, nz // tile, body, 0, unroll=4)

    apply_inverse(inv[...], bs, u0s, nz, 4, 4)
    spread(u0s, g1s)
    apply_inverse(inv[...], g1s, u1s, nz, 4, 4)
    spread(u1s, g2s)
    apply_inverse(inv[...], g2s, u2s, nz, 4, 4)
    lane8 = lane_ids(tile)
    pos8 = lax.rem(lane8, GROUP)
    rows = (lane8 >= GROUP * STEPS) & (lane8 < GROUP * (STEPS + nx // 2))

    def body(i, sums):
        k = i * tile
        at_b, at_0, at_1, at_2, at_f1, at_f2 = (rows_at(ref, k, tile, nz) for ref in (bs, u0s, u1s, u2s, g1s, g2s))
        h = h_wide[pl.ds(pl.multiple_of(k, 8), tile), :]
        part = [None, None]
        for j in range(4):
            v2 = at_2(j)
            f3 = h * (sideways(v2) + sideways(v2, GROUP))
            g3s[pl.ds(pl.multiple_of(j * nz + k, 8), tile), :] = f3
            terms = inner_terms(at_b(j), at_f1(j), at_f2(j), f3, at_0(j), at_1(j), v2)
            part[j // 2] = terms if part[j // 2] is None else add_all(part[j // 2], terms)
        mine = tuple(
            jnp.where(rows & (pos8 >= STEPS) & (pos8 < 2 * STEPS), p, jnp.where(rows & (pos8 < STEPS), q, 0.0))
            for p, q in zip(*part)
        )
        return add_all(sums, mine)

    sums = tuple(sums_in[8 * i : 8 * i + 8, :] for i in range(9))
    sums = lax.fori_loop(0, nz // tile, body, sums)
    out = jnp.zeros((8, LANES), F32)
    for i, s in enumerate(sums):
        total = jnp.sum(jnp.sum(s, axis=0, keepdims=True), axis=1, keepdims=True)
        out = jnp.where(lane8 == i, jnp.broadcast_to(total, (8, LANES)), out)
    for i in range(members // 8):
        send[8 * i : 8 * i + 8, :] = out


def fold(v):
    out = v[0:8]
    for i in range(1, v.shape[0] // 8):
        out = out + v[8 * i : 8 * i + 8]
    return out


def solve_small(t):
    g00, g10, g11, g20, g21, g22, m0, m1, m2 = t
    l1, l2 = g10 / g00, g20 / g00
    d1 = g11 - l1 * g10
    e = g21 - l2 * g10
    l3 = e / d1
    d2 = g22 - l2 * g20 - l3 * e
    y1 = m1 - l1 * m0
    y2 = m2 - l2 * m0 - l3 * y1
    c2 = y2 / d2
    c1 = y1 / d1 - l3 * c2
    return m0 / g00 - l1 * c1 - l2 * c2, c1, c2


def combine_kernel(nz, nx, kz, *refs):
    got, fields, strips, outs, coef = refs[0], refs[1:8], refs[8:15], refs[15:17], refs[17]
    step = pl.program_id(0)

    @pl.when(step == 0)
    def _():
        total = jnp.sum(fold(got[...]), axis=0, keepdims=True)
        line = lax.broadcasted_iota(jnp.int32, (1, LANES), 1)
        pick = lambda i: jnp.sum(jnp.where(line == i, total, 0.0), axis=1, keepdims=True)
        for i, c in enumerate(solve_small([pick(i) for i in range(9)])):
            coef[i * 8 : i * 8 + 8, :] = jnp.broadcast_to(c, (8, LANES))

    c0, c1, c2 = (jnp.concatenate([coef[i * 8 : i * 8 + 8, :]] * (kz // 8), axis=0) for i in range(3))
    lane = lane_ids(kz)
    inside = (lane >= STEPS) & (lane < LANES - STEPS)
    pos = lax.rem(lane, GROUP)

    def combined(b, v0, v1, v2, f1, f2, f3):
        return c0 * v0 + c1 * v1 + c2 * v2, b - (c0 * (b - f1) + c1 * (f1 - f2) + c2 * (f2 - f3))

    def at(ref, r):
        return ref[pl.ds(pl.multiple_of(r * nz + step * kz, 8), kz), :]

    edges = []
    for t in range(2):
        near, far = combined(*(at(ref, t) for ref in strips)), combined(*(at(ref, t + 2) for ref in strips))
        edges.append([jnp.where(pos >= STEPS, p, q) for p, q in zip(near, far)])
    for t, x, group in strip_places(nx):
        if not t * (nx // 2) <= x < (t + 1) * (nx // 2):
            continue
        values = combined(*(at(ref, x + skip) for ref, skip in zip(fields, (0, 3, 2, 1, 2, 1, 0))))
        for out, value, edge in zip(outs, values, edges[t]):
            turned = pltpu.roll(edge, (-(GROUP * group + STEPS)) % LANES, 1)
            out[pl.ds(x, kz, stride=nx), :] = jnp.where(inside, value, turned)


def neighbours(array, axes, up):
    size = lax.axis_size(axes)
    pairs = [(i, (i + 1) % size) for i in range(size)]
    return lax.ppermute(array, axes, pairs if up else [(b, a) for a, b in pairs])


def on_device(source_heat, horiz_coef, face_coef, column_inverse):
    nz, nx, ny = source_heat.shape
    gx, gy = "gx", "gy"
    members = lax.axis_size(gx) * lax.axis_size(gy)
    part = lambda f, *a: (lambda *refs: f(*a, *refs))
    nat = source_heat.reshape(nz * nx, ny)
    low, high = pl.pallas_call(
        part(load_kernel, nz, nx),
        in_specs=[spec()],
        out_specs=[spec()] * 2,
        out_shape=[vmem(STEPS * nz)] * 2,
        compiler_params=params(4),
    )(nat)
    below = neighbours(high, gx, True)
    above = neighbours(low, gx, False)
    b_t, u0, h_wide, inner_own, outer_own = pl.pallas_call(
        part(own_kernel, nz, nx),
        in_specs=[spec()] * 3,
        out_specs=[spec()] * 5,
        out_shape=[vmem(nz * nx), vmem(nz * nx), vmem(nz), vmem(2 * nz), vmem(2 * nz)],
        compiler_params=params(8),
        cost_estimate=cost(12 * nz * nz * nx * ny, 1 << 20),
    )(nat, horiz_coef.reshape(1, nz), column_inverse)
    inner, outer = pl.pallas_call(
        part(pack_kernel, nz, nx),
        in_specs=[spec()] * 4,
        out_specs=[spec()] * 2,
        out_shape=[vmem(2 * nz)] * 2,
        compiler_params=params(4),
    )(inner_own, outer_own, below, above)
    from_left = neighbours(inner, gy, True)
    from_right = neighbours(inner, gy, False)
    u0e, u1e, u2e, g1e, g2e, g3, sums = pl.pallas_call(
        part(main_kernel, nz, nx),
        in_specs=[spec()] * 6,
        out_specs=[spec()] * 7,
        out_shape=[vmem(r * nz) for r in (nx + 6, nx + 4, nx + 2, nx + 4, nx + 2, nx)] + [vmem(72)],
        compiler_params=params(12),
        cost_estimate=cost(36 * nz * nz * nx * ny, 1 << 20),
    )(b_t, u0, below, above, column_inverse, h_wide)
    *strips, send = pl.pallas_call(
        part(strip_kernel, nz, nx, members),
        in_specs=[spec()] * 7,
        out_specs=[spec()] * 8,
        out_shape=[vmem(4 * nz)] * 7 + [vmem(members)],
        compiler_params=params(8),
    )(inner, outer, from_left, from_right, column_inverse, h_wide, sums)
    got = lax.all_to_all(send.reshape(members, 1, LANES), (gx, gy), split_axis=0, concat_axis=0, tiled=True)
    kz = 32
    pressure, true_residual = pl.pallas_call(
        part(combine_kernel, nz, nx, kz),
        grid=(nz // kz,),
        in_specs=[spec()] * 15,
        out_specs=[pl.BlockSpec((kz * nx, ny), lambda i: (i, 0))] * 2,
        out_shape=[jax.ShapeDtypeStruct((nz * nx, ny), F32)] * 2,
        scratch_shapes=[pltpu.VMEM((24, LANES), F32)],
        compiler_params=params(8),
    )(got.reshape(members, LANES), b_t, u0e, u1e, u2e, g1e, g2e, g3, *strips)
    return pressure.reshape(nz, nx, ny), true_residual.reshape(nz, nx, ny)


def solution(mesh):
    field = P(None, "gx", "gy")
    return jax.shard_map(
        on_device,
        mesh=mesh,
        in_specs=(field, P(), P(), P()),
        out_specs=(field, field),
        check_vma=False,
    )
```

```python
import jax
import jax.numpy as jnp
from jax import lax
from jax.experimental import pallas as pl
from jax.experimental.pallas import tpu as pltpu
from jax.sharding import Mesh
from jax.sharding import PartitionSpec as P

F32 = jnp.float32
BF16 = jnp.bfloat16
LANES = 128
GROUP = 9
STEPS = 3
WIDTH = 4


def vmem(rows, cols=LANES):
    return pltpu.VMEM((rows, cols), F32)


def spec():
    return pl.BlockSpec(memory_space=pltpu.VMEM)


def params(mib):
    return pltpu.CompilerParams(vmem_limit_bytes=mib * 1024 * 1024)


def cost(flops, size):
    return pl.CostEstimate(flops=flops, bytes_accessed=size, transcendentals=0)


def lane_ids(rows):
    return lax.broadcasted_iota(jnp.int32, (rows, LANES), 1)


def pieces(v):
    high = v.astype(BF16)
    rest = v - high.astype(F32)
    middle = rest.astype(BF16)
    return high, middle, (rest - middle.astype(F32)).astype(BF16)


def product(factors, columns):
    nz = columns.shape[0]
    stacked = jnp.concatenate(pieces(columns), axis=0)
    dot = lambda f, count: jnp.dot(f[...], stacked[: count * nz], preferred_element_type=F32)
    return dot(factors[0], 3) + dot(factors[1], 2) + dot(factors[2], 1)


def apply_inverse(factors, src, dst, nz, tiles, width):
    for first in range(0, tiles, width):
        count = min(width, tiles - first)
        parts = [src[(first + t) * nz : (first + t + 1) * nz, :] for t in range(count)]
        out = product(factors, jnp.concatenate(parts, axis=1) if count > 1 else parts[0])
        for t in range(count):
            dst[(first + t) * nz : (first + t + 1) * nz, :] = out[:, t * LANES : (t + 1) * LANES]


def load_kernel(nz, nx, nat, inv, low, high, inv_out):
    inv_out[...] = inv[...]
    for i in range(STEPS):
        low[i * nz : (i + 1) * nz, :] = nat[pl.ds(i, nz, stride=nx), :]
        high[i * nz : (i + 1) * nz, :] = nat[pl.ds(nx - STEPS + i, nz, stride=nx), :]


def place(lane):
    return lane - GROUP * lax.shift_right_logical(lane * 57, 9)


def strip_places(nx):
    half = nx // 2
    count = half + 2 * STEPS
    return [(t, t * half - STEPS + r, r) for t in range(2) for r in range(count)]


def add_edges(row, group, lane, inner, outer):
    first = GROUP * group
    turned = pltpu.roll(row, (first + STEPS) % LANES, 1)
    inner = jnp.where((lane >= first) & (lane < first + GROUP), turned, inner)
    if first:
        mine = (lane >= first - STEPS) & (lane < first + 2 * STEPS)
    else:
        mine = (lane >= LANES - STEPS) | (lane < 2 * STEPS)
    outer = jnp.where(mine, turned, outer)
    return inner, outer


def pack_edges(rows, first_x, nx, nz, inner, outer, tile, fresh):
    lane = lane_ids(tile)
    wanted, have = rows

    def body(i, carry):
        k = i * tile
        for t in range(2):
            at = pl.ds(pl.multiple_of(t * nz + k, 8), tile)
            if fresh:
                packed = (jnp.zeros((tile, LANES), F32),) * 2
            else:
                packed = (inner[at, :], outer[at, :])
            for u, x, group in strip_places(nx):
                if u == t and x in wanted:
                    packed = add_edges(have(x, k), group, lane, *packed)
            inner[at, :], outer[at, :] = packed
        return carry

    lax.fori_loop(0, nz // tile, body, 0, unroll=4 if fresh else True)


def own_kernel(nz, nx, nat, h_row, inv, b_t, u0, h_wide, inner, outer, *factors):
    for ref, piece, count in zip(factors, pieces(inv[...]), (3, 2, 1)):
        wide = piece.astype(F32)
        ref[...] = jnp.concatenate([wide] * count, axis=1).astype(BF16) if count > 1 else piece
    eye = lax.broadcasted_iota(jnp.int32, (nz, nz), 0) == lax.broadcasted_iota(jnp.int32, (nz, nz), 1)
    column = jnp.sum(jnp.where(eye, jnp.broadcast_to(h_row[...], (nz, nz)), 0.0), axis=1, keepdims=True)
    h_wide[...] = jnp.broadcast_to(column, (nz, LANES))
    for x in range(nx):
        b_t[x * nz : (x + 1) * nz, :] = nat[pl.ds(x, nz, stride=nx), :]
    have = lambda x, k: b_t[pl.ds(pl.multiple_of(x * nz + k, 8), 8), :]
    pack_edges((range(nx), have), 0, nx, nz, inner, outer, 8, True)
    apply_inverse(factors, b_t, u0, nz, nx, nx)


def pack_kernel(nz, nx, inner_own, outer_own, below, above, inner, outer):
    inner[...] = inner_own[...]
    outer[...] = outer_own[...]

    def have(x, k):
        ref, r = (below, x + STEPS) if x < 0 else (above, x - nx)
        return ref[pl.ds(pl.multiple_of(r * nz + k, 8), 8), :]

    wanted = [*range(-STEPS, 0), *range(nx, nx + STEPS)]
    pack_edges((wanted, have), -STEPS, nx, nz, inner, outer, 8, False)


def sideways(mid, step=1):
    return pltpu.roll(mid, step, 1) + pltpu.roll(mid, LANES - step, 1)


class Sums:
    def __init__(self):
        self.total = {}

    def add(self, terms):
        for name in terms[0]:
            row = terms[0][name]
            for more in terms[1:]:
                row = row + more[name]
            self.total[name] = row if name not in self.total else self.total[name] + row


NAMES = ("00", "10", "11", "20", "21", "22", "0b", "1b", "2b")


def stage_terms(level, b, gs, v):
    chain = (b, *gs)
    out = {f"{level}{j}": v * (chain[j] - chain[j + 1]) for j in range(level + 1)}
    out[f"{level}b"] = v * b
    return out


def advance(factors, neighbours_of, g, u, h_ref, nz, count, width, visit, tile=8):
    for first in range(0, count, width):
        rows = []
        for j in range(first, min(first + width, count)):
            parts, terms = [], []
            for k in range(0, nz, tile):
                parts.append(h_ref[k : k + tile, :] * neighbours_of(j, k))
                found = visit(j, k, parts[-1])
                if found:
                    terms.append(found)
            visit.finish(j, terms)
            rows.append(jnp.concatenate(parts, axis=0))
            g[j * nz : (j + 1) * nz, :] = rows[-1]
        if u is None:
            continue
        out = product(factors, jnp.concatenate(rows, axis=1) if len(rows) > 1 else rows[0])
        for t in range(len(rows)):
            u[(first + t) * nz : (first + t + 1) * nz, :] = out[:, t * LANES : (t + 1) * LANES]


class Visit:
    def __init__(self, level, nz, fields, rows, sums_of):
        self.level, self.nz, self.fields, self.rows, self.sums_of = level, nz, fields, rows, sums_of

    def __call__(self, j, k, g):
        x = self.rows(j)
        if x is None:
            return None
        b, *gs, v = (ref[(x + skip) * self.nz + k : (x + skip) * self.nz + k + 8, :] for ref, skip in self.fields)
        return stage_terms(self.level, b, (*gs, g), v)

    def finish(self, j, terms):
        if terms:
            self.sums_of(j).add(terms)


def main_kernel(nz, nx, b_t, u0, below, above, h_wide, f0, f1, f2, u0e, u1e, u2e, g1e, g2e, g3, sums_out):
    u0e[STEPS * nz : (STEPS + nx) * nz, :] = u0[...]
    factors = (f0, f1, f2)
    for ref, first in ((below, 0), (above, STEPS + nx)):
        apply_inverse(factors, ref, u0e.at[pl.ds(first * nz, STEPS * nz), :], nz, STEPS, STEPS)
    sums = Sums()

    def around(v):
        def of(j, k):
            at = lambda r: v[r * nz + k : r * nz + k + 8, :]
            return (at(j) + at(j + 2)) + sideways(at(j + 1))

        return of

    inside = lambda extra: (lambda j: j - extra if 0 <= j - extra < nx else None)
    b_f, f1_f, f2_f = (b_t, 0), (g1e, 2), (g2e, 1)
    one = Visit(0, nz, (b_f, (u0e, 3)), inside(2), lambda j: sums)
    advance(factors, around(u0e), g1e, u1e, h_wide, nz, nx + 4, WIDTH, one)
    two = Visit(1, nz, (b_f, f1_f, (u1e, 2)), inside(1), lambda j: sums)
    advance(factors, around(u1e), g2e, u2e, h_wide, nz, nx + 2, WIDTH, two)
    three = Visit(2, nz, (b_f, f1_f, f2_f, (u2e, 1)), inside(0), lambda j: sums)
    advance(factors, around(u2e), g3, None, h_wide, nz, nx, WIDTH, three)
    lane = lane_ids(8)
    for i, name in enumerate(NAMES):
        sums_out[8 * i : 8 * i + 8, :] = jnp.where((lane >= STEPS) & (lane < LANES - STEPS), sums.total[name], 0.0)


def strip_kernel(nz, nx, members, inner, outer, left, right, h_wide, sums_in, f0, f1, f2, bs, u0s, u1s, u2s, g1s, g2s, g3s, send):
    factors = (f0, f1, f2)
    lane = lane_ids(nz)
    pos = place(lane)
    used = lane < GROUP * (nx // 2 + 2 * STEPS)
    for t in range(2):
        at = slice(t * nz, (t + 1) * nz)
        bs[t * nz : (t + 1) * nz, :] = jnp.where((pos < STEPS) & used, left[at, :], inner[at, :])
        bs[(t + 2) * nz : (t + 3) * nz, :] = jnp.where((pos >= STEPS) & (pos < 2 * STEPS) & used, right[at, :], outer[at, :])
    near, far = Sums(), Sums()
    sums_of = lambda j: near if j < 2 else far

    def around(v):
        def of(j, k):
            mid = v[j * nz + k : j * nz + k + 8, :]
            return sideways(mid) + sideways(mid, GROUP)

        return of

    every = lambda j: j
    apply_inverse(factors, bs, u0s, nz, 4, 4)
    advance(factors, around(u0s), g1s, u1s, h_wide, nz, 4, 4, Visit(0, nz, ((bs, 0), (u0s, 0)), every, sums_of))
    advance(factors, around(u1s), g2s, u2s, h_wide, nz, 4, 4, Visit(1, nz, ((bs, 0), (g1s, 0), (u1s, 0)), every, sums_of))
    last = Visit(2, nz, ((bs, 0), (g1s, 0), (g2s, 0), (u2s, 0)), every, sums_of)
    advance(factors, around(u2s), g3s, None, h_wide, nz, 4, 4, last)
    lane = lane_ids(8)
    pos = place(lane)
    rows = (lane >= GROUP * STEPS) & (lane < GROUP * (STEPS + nx // 2))
    out = jnp.zeros((8, LANES), F32)
    for i, name in enumerate(NAMES):
        p = jnp.where(rows & (pos >= STEPS) & (pos < 2 * STEPS), near.total[name], 0.0)
        q = jnp.where(rows & (pos < STEPS), far.total[name], 0.0)
        s = sums_in[8 * i : 8 * i + 8, :] + (p + q)
        total = jnp.sum(jnp.sum(s, axis=0, keepdims=True), axis=1, keepdims=True)
        out = jnp.where(lane == i, jnp.broadcast_to(total, (8, LANES)), out)
    for i in range(members // 8):
        send[8 * i : 8 * i + 8, :] = out


def fold(v):
    out = v[0:8]
    for i in range(1, v.shape[0] // 8):
        out = out + v[8 * i : 8 * i + 8]
    return out


def solve_small(t):
    g00, g10, g11, g20, g21, g22, m0, m1, m2 = t
    l1, l2 = g10 / g00, g20 / g00
    d1 = g11 - l1 * g10
    e = g21 - l2 * g10
    l3 = e / d1
    d2 = g22 - l2 * g20 - l3 * e
    y1 = m1 - l1 * m0
    y2 = m2 - l2 * m0 - l3 * y1
    c2 = y2 / d2
    c1 = y1 / d1 - l3 * c2
    return m0 / g00 - l1 * c1 - l2 * c2, c1, c2


def combine_kernel(nz, nx, kz, *refs):
    got, fields, strips, outs, coef = refs[0], refs[1:8], refs[8:15], refs[15:17], refs[17]
    step = pl.program_id(0)

    @pl.when(step == 0)
    def _():
        total = jnp.sum(fold(got[...]), axis=0, keepdims=True)
        line = lax.broadcasted_iota(jnp.int32, (1, LANES), 1)
        pick = lambda i: jnp.sum(jnp.where(line == i, total, 0.0), axis=1, keepdims=True)
        for i, c in enumerate(solve_small([pick(i) for i in range(9)])):
            coef[i * 8 : i * 8 + 8, :] = jnp.broadcast_to(c, (8, LANES))

    c0, c1, c2 = (jnp.concatenate([coef[i * 8 : i * 8 + 8, :]] * (kz // 8), axis=0) for i in range(3))
    lane = lane_ids(kz)
    inside = (lane >= STEPS) & (lane < LANES - STEPS)
    pos = place(lane)

    def combined(b, v0, v1, v2, f1, f2, f3):
        return c0 * v0 + c1 * v1 + c2 * v2, b - (c0 * (b - f1) + c1 * (f1 - f2) + c2 * (f2 - f3))

    def at(ref, r):
        return ref[pl.ds(pl.multiple_of(r * nz + step * kz, 8), kz), :]

    edges = []
    for t in range(2):
        near, far = combined(*(at(ref, t) for ref in strips)), combined(*(at(ref, t + 2) for ref in strips))
        edges.append([jnp.where(pos >= STEPS, p, q) for p, q in zip(near, far)])
    for t, x, group in strip_places(nx):
        if not t * (nx // 2) <= x < (t + 1) * (nx // 2):
            continue
        values = combined(*(at(ref, x + skip) for ref, skip in zip(fields, (0, 3, 2, 1, 2, 1, 0))))
        for out, value, edge in zip(outs, values, edges[t]):
            turned = pltpu.roll(edge, (-(GROUP * group + STEPS)) % LANES, 1)
            out[pl.ds(x, kz, stride=nx), :] = jnp.where(inside, value, turned)


def neighbours(array, axes, up):
    size = lax.axis_size(axes)
    pairs = [(i, (i + 1) % size) for i in range(size)]
    return lax.ppermute(array, axes, pairs if up else [(b, a) for a, b in pairs])


def on_device(source_heat, horiz_coef, face_coef, column_inverse):
    nz, nx, ny = source_heat.shape
    gx, gy = "gx", "gy"
    members = lax.axis_size(gx) * lax.axis_size(gy)
    part = lambda f, *a: (lambda *refs: f(*a, *refs))
    nat = source_heat.reshape(nz * nx, ny)
    low, high, inv = pl.pallas_call(
        part(load_kernel, nz, nx),
        in_specs=[spec()] * 2,
        out_specs=[spec()] * 3,
        out_shape=[vmem(STEPS * nz)] * 2 + [vmem(nz, nz)],
        compiler_params=params(4),
    )(nat, column_inverse)
    below = neighbours(high, gx, True)
    above = neighbours(low, gx, False)
    b_t, u0, h_wide, inner_own, outer_own, *factors = pl.pallas_call(
        part(own_kernel, nz, nx),
        in_specs=[spec()] * 3,
        out_specs=[spec()] * 8,
        out_shape=[vmem(nz * nx), vmem(nz * nx), vmem(nz), vmem(2 * nz), vmem(2 * nz)]
        + [pltpu.VMEM((nz, count * nz), BF16) for count in (3, 2, 1)],
        compiler_params=params(8),
        cost_estimate=cost(12 * nz * nz * nx * ny, 1 << 20),
    )(nat, horiz_coef.reshape(1, nz), inv)
    inner, outer = pl.pallas_call(
        part(pack_kernel, nz, nx),
        in_specs=[spec()] * 4,
        out_specs=[spec()] * 2,
        out_shape=[vmem(2 * nz)] * 2,
        compiler_params=params(4),
    )(inner_own, outer_own, below, above)
    from_left = neighbours(inner, gy, True)
    from_right = neighbours(inner, gy, False)
    u0e, u1e, u2e, g1e, g2e, g3, sums = pl.pallas_call(
        part(main_kernel, nz, nx),
        in_specs=[spec()] * 8,
        out_specs=[spec()] * 7,
        out_shape=[vmem(r * nz) for r in (nx + 6, nx + 4, nx + 2, nx + 4, nx + 2, nx)] + [vmem(72)],
        compiler_params=params(12),
        cost_estimate=cost(36 * nz * nz * nx * ny, 1 << 20),
    )(b_t, u0, below, above, h_wide, *factors)
    *strips, send = pl.pallas_call(
        part(strip_kernel, nz, nx, members),
        in_specs=[spec()] * 9,
        out_specs=[spec()] * 8,
        out_shape=[vmem(4 * nz)] * 7 + [vmem(members)],
        compiler_params=params(8),
    )(inner, outer, from_left, from_right, h_wide, sums, *factors)
    got = lax.all_to_all(send.reshape(members, 1, LANES), (gx, gy), split_axis=0, concat_axis=0, tiled=True)
    kz = 80
    pressure, true_residual = pl.pallas_call(
        part(combine_kernel, nz, nx, kz),
        grid=(nz // kz,),
        in_specs=[spec()] * 15,
        out_specs=[pl.BlockSpec((kz * nx, ny), lambda i: (i, 0))] * 2,
        out_shape=[jax.ShapeDtypeStruct((nz * nx, ny), F32)] * 2,
        scratch_shapes=[pltpu.VMEM((24, LANES), F32)],
        compiler_params=params(8),
    )(got.reshape(members, LANES), b_t, u0e, u1e, u2e, g1e, g2e, g3, *strips)
    return pressure.reshape(nz, nx, ny), true_residual.reshape(nz, nx, ny)


def solution(mesh):
    field = P(None, "gx", "gy")
    return jax.shard_map(
        on_device,
        mesh=mesh,
        in_specs=(field, P(), P(), P()),
        out_specs=(field, field),
        check_vma=False,
    )
```

```python
import jax
import jax.numpy as jnp
from jax import lax
from jax.experimental import pallas as pl
from jax.experimental.pallas import tpu as pltpu
from jax.sharding import Mesh
from jax.sharding import PartitionSpec as P

F32 = jnp.float32
BF16 = jnp.bfloat16
LANES = 128
GROUP = 9
STEPS = 3
WIDTH = 4
WIDE = 3
BLOCK = 32


def vmem(rows, cols=LANES):
    return pltpu.VMEM((rows, cols), F32)


def spec():
    return pl.BlockSpec(memory_space=pltpu.VMEM)


def params(mib):
    return pltpu.CompilerParams(vmem_limit_bytes=mib * 1024 * 1024)


def cost(flops, size):
    return pl.CostEstimate(flops=flops, bytes_accessed=size, transcendentals=0)


def lane_ids(rows):
    return lax.broadcasted_iota(jnp.int32, (rows, LANES), 1)


def pieces(v):
    high = v.astype(BF16)
    rest = v - high.astype(F32)
    middle = rest.astype(BF16)
    return high, middle, (rest - middle.astype(F32)).astype(BF16)


def product(factors, columns):
    nz = columns.shape[0]
    stacked = jnp.concatenate(pieces(columns), axis=0)
    dot = lambda f, count: jnp.dot(f[...], stacked[: count * nz], preferred_element_type=F32)
    return dot(factors[0], 3) + dot(factors[1], 2) + dot(factors[2], 1)


def apply_inverse(factors, src, dst, nz, tiles, width):
    for first in range(0, tiles, width):
        count = min(width, tiles - first)
        parts = [src[(first + t) * nz : (first + t + 1) * nz, :] for t in range(count)]
        out = product(factors, jnp.concatenate(parts, axis=1) if count > 1 else parts[0])
        for t in range(count):
            dst[(first + t) * nz : (first + t + 1) * nz, :] = out[:, t * LANES : (t + 1) * LANES]


def load_kernel(nz, nx, nat, low, high):
    for i in range(STEPS):
        low[i * nz : (i + 1) * nz, :] = nat[pl.ds(i, nz, stride=nx), :]
        high[i * nz : (i + 1) * nz, :] = nat[pl.ds(nx - STEPS + i, nz, stride=nx), :]


def place(lane):
    return lane - GROUP * lax.shift_right_logical(lane * 57, 9)


def strip_places(nx):
    half = nx // 2
    count = half + 2 * STEPS
    return [(t, t * half - STEPS + r, r) for t in range(2) for r in range(count)]


def add_edges(row, group, lane, inner, outer):
    first = GROUP * group
    turned = pltpu.roll(row, (first + STEPS) % LANES, 1)
    inner = jnp.where((lane >= first) & (lane < first + GROUP), turned, inner)
    if first:
        mine = (lane >= first - STEPS) & (lane < first + 2 * STEPS)
    else:
        mine = (lane >= LANES - STEPS) | (lane < 2 * STEPS)
    outer = jnp.where(mine, turned, outer)
    return inner, outer


def pack_edges(rows, first_x, nx, nz, inner, outer, tile, fresh):
    lane = lane_ids(tile)
    wanted, have = rows

    def body(i, carry):
        k = i * tile
        for t in range(2):
            at = pl.ds(pl.multiple_of(t * nz + k, 8), tile)
            if fresh:
                packed = (jnp.zeros((tile, LANES), F32),) * 2
            else:
                packed = (inner[at, :], outer[at, :])
            for u, x, group in strip_places(nx):
                if u == t and x in wanted:
                    packed = add_edges(have(x, k), group, lane, *packed)
            inner[at, :], outer[at, :] = packed
        return carry

    lax.fori_loop(0, nz // tile, body, 0, unroll=4 if fresh else True)


def own_kernel(nz, nx, nat, h_row, inv, b_t, u0, h_wide, inner, outer, *factors):
    for ref, piece, count in zip(factors, pieces(inv[...]), (3, 2, 1)):
        wide = piece.astype(F32)
        ref[...] = jnp.concatenate([wide] * count, axis=1).astype(BF16) if count > 1 else piece
    eye = lax.broadcasted_iota(jnp.int32, (nz, nz), 0) == lax.broadcasted_iota(jnp.int32, (nz, nz), 1)
    column = jnp.sum(jnp.where(eye, jnp.broadcast_to(h_row[...], (nz, nz)), 0.0), axis=1, keepdims=True)
    h_wide[...] = jnp.broadcast_to(column, (nz, LANES))
    for x in range(nx):
        b_t[x * nz : (x + 1) * nz, :] = nat[pl.ds(x, nz, stride=nx), :]
    have = lambda x, k: b_t[pl.ds(pl.multiple_of(x * nz + k, 8), 8), :]
    pack_edges((range(nx), have), 0, nx, nz, inner, outer, 8, True)
    apply_inverse(factors, b_t, u0, nz, nx, nx)


def pack_kernel(nz, nx, inner_own, outer_own, below, above, inner, outer):
    inner[...] = inner_own[...]
    outer[...] = outer_own[...]

    def have(x, k):
        ref, r = (below, x + STEPS) if x < 0 else (above, x - nx)
        return ref[pl.ds(pl.multiple_of(r * nz + k, 8), 8), :]

    wanted = [*range(-STEPS, 0), *range(nx, nx + STEPS)]
    pack_edges((wanted, have), -STEPS, nx, nz, inner, outer, 8, False)


def sideways(mid, step=1):
    return pltpu.roll(mid, step, 1) + pltpu.roll(mid, LANES - step, 1)


class Sums:
    def __init__(self):
        self.total = {}

    def add(self, terms):
        for name in terms[0]:
            row = terms[0][name]
            for more in terms[1:]:
                row = row + more[name]
            self.total[name] = row if name not in self.total else self.total[name] + row


NAMES = ("00", "10", "11", "20", "21", "22", "0b", "1b", "2b")


def stage_terms(level, b, gs, v):
    chain = (b, *gs)
    out = {f"{level}{j}": v * (chain[j] - chain[j + 1]) for j in range(level + 1)}
    out[f"{level}b"] = v * b
    return out


class Field:
    def __init__(self, nz, *places):
        self.nz = nz
        self.where = {x: (ref, i) for ref, xs in places for i, x in enumerate(xs)}

    def at(self, x, k, size=8):
        ref, i = self.where[x]
        return ref[i * self.nz + k : i * self.nz + k + size, :]


def advance(factors, xs, u_last, around, g, u, h_ref, width, visit, tile=8):
    nz = u_last.nz
    for first in range(0, len(xs), width):
        rows = []
        for i, x in enumerate(xs[first : first + width], first):
            parts, terms = [], []
            for k in range(0, nz, tile):
                parts.append(h_ref[k : k + tile, :] * around(u_last, x, k))
                found = visit(x, k, parts[-1])
                if found:
                    terms.append(found)
            visit.finish(x, terms)
            rows.append(jnp.concatenate(parts, axis=0))
            g[i * nz : (i + 1) * nz, :] = rows[-1]
        if u is None:
            continue
        out = product(factors, jnp.concatenate(rows, axis=1) if len(rows) > 1 else rows[0])
        for t in range(len(rows)):
            u[(first + t) * nz : (first + t + 1) * nz, :] = out[:, t * LANES : (t + 1) * LANES]


def five_points(v, x, k):
    return (v.at(x - 1, k) + v.at(x + 1, k)) + sideways(v.at(x, k))


def packed_points(v, x, k):
    mid = v.at(x, k)
    return sideways(mid) + sideways(mid, GROUP)


class Visit:
    def __init__(self, level, fields, mine, sums_of):
        self.level, self.fields, self.mine, self.sums_of = level, fields, mine, sums_of

    def __call__(self, x, k, g):
        if x not in self.mine:
            return None
        b, *gs, v = (field.at(x, k) for field in self.fields)
        return stage_terms(self.level, b, (*gs, g), v)

    def finish(self, x, terms):
        if terms:
            self.sums_of(x).add(terms)


def inner_rows(nx, level):
    return list(range(level, nx - level))


def outer_rows(nx, level):
    low = list(range(level - STEPS, level))
    return low + [nx - 1 - x for x in reversed(low)]


def store_sums(sums, out, start=None):
    lane = lane_ids(8)
    for i, name in enumerate(NAMES):
        at = slice(8 * i, 8 * i + 8)
        s = jnp.where((lane >= STEPS) & (lane < LANES - STEPS), sums.total[name], 0.0)
        out[at, :] = s if start is None else start[at, :] + s


def inner_kernel(nz, nx, b_t, u0, h_wide, f0, f1, f2, g1i, u1i, g2i, u2i, g3i, sums_out):
    factors, every, sums = (f0, f1, f2), range(nx), Sums()
    b, v0 = Field(nz, (b_t, every)), Field(nz, (u0, every))
    rows = [inner_rows(nx, level) for level in range(STEPS + 1)]
    v1, v2 = Field(nz, (u1i, rows[1])), Field(nz, (u2i, rows[2]))
    e1, e2 = Field(nz, (g1i, rows[1])), Field(nz, (g2i, rows[2]))
    count = lambda level, *fields: Visit(level, fields, every, lambda x: sums)
    advance(factors, rows[1], v0, five_points, g1i, u1i, h_wide, WIDTH, count(0, b, v0))
    advance(factors, rows[2], v1, five_points, g2i, u2i, h_wide, WIDTH, count(1, b, e1, v1))
    advance(factors, rows[3], v2, five_points, g3i, None, h_wide, WIDTH, count(2, b, e1, e2, v2))
    store_sums(sums, sums_out)


def outer_kernel(nz, nx, b_t, u0, below, above, h_wide, f0, f1, f2, g1i, u1i, g2i, u2i, start, *outs):
    u0x, g1x, u1x, g2x, u2x, g3x, sums_out = outs
    factors, every, sums = (f0, f1, f2), range(nx), Sums()
    half = STEPS * nz
    out = product(factors, jnp.concatenate([ref[i * nz : (i + 1) * nz, :] for ref in (below, above) for i in range(STEPS)], axis=1))
    for i in range(2 * STEPS):
        u0x[i * nz : (i + 1) * nz, :] = out[:, i * LANES : (i + 1) * LANES]
    inner = [inner_rows(nx, level) for level in range(STEPS + 1)]
    outer = [outer_rows(nx, level) for level in range(STEPS + 1)]
    both = lambda level, i, x: Field(nz, (i, inner[level]), (x, outer[level]))
    b, v0, v1, v2 = Field(nz, (b_t, every)), both(0, u0, u0x), both(1, u1i, u1x), both(2, u2i, u2x)
    e1, e2 = both(1, g1i, g1x), both(2, g2i, g2x)
    count = lambda level, *fields: Visit(level, fields, every, lambda x: sums)
    advance(factors, outer[1], v0, five_points, g1x, u1x, h_wide, WIDE, count(0, b, v0))
    advance(factors, outer[2], v1, five_points, g2x, u2x, h_wide, WIDE, count(1, b, e1, v1))
    advance(factors, outer[3], v2, five_points, g3x, None, h_wide, WIDE, count(2, b, e1, e2, v2))
    store_sums(sums, sums_out, start)


def strip_kernel(nz, nx, members, inner, outer, left, right, h_wide, sums_in, f0, f1, f2, bs, u0s, u1s, u2s, g1s, g2s, g3s, send):
    factors = (f0, f1, f2)
    lane = lane_ids(nz)
    pos = place(lane)
    used = lane < GROUP * (nx // 2 + 2 * STEPS)
    for t in range(2):
        at = slice(t * nz, (t + 1) * nz)
        bs[t * nz : (t + 1) * nz, :] = jnp.where((pos < STEPS) & used, left[at, :], inner[at, :])
        bs[(t + 2) * nz : (t + 3) * nz, :] = jnp.where((pos >= STEPS) & (pos < 2 * STEPS) & used, right[at, :], outer[at, :])
    near, far, tiles = Sums(), Sums(), list(range(4))
    field = lambda ref: Field(nz, (ref, tiles))
    count = lambda level, *refs: Visit(level, [field(ref) for ref in refs], tiles, lambda j: near if j < 2 else far)
    apply_inverse(factors, bs, u0s, nz, 4, 4)
    advance(factors, tiles, field(u0s), packed_points, g1s, u1s, h_wide, 4, count(0, bs, u0s))
    advance(factors, tiles, field(u1s), packed_points, g2s, u2s, h_wide, 4, count(1, bs, g1s, u1s))
    advance(factors, tiles, field(u2s), packed_points, g3s, None, h_wide, 4, count(2, bs, g1s, g2s, u2s))
    lane = lane_ids(8)
    pos = place(lane)
    rows = (lane >= GROUP * STEPS) & (lane < GROUP * (STEPS + nx // 2))
    out = jnp.zeros((8, LANES), F32)
    for i, name in enumerate(NAMES):
        p = jnp.where(rows & (pos >= STEPS) & (pos < 2 * STEPS), near.total[name], 0.0)
        q = jnp.where(rows & (pos < STEPS), far.total[name], 0.0)
        s = sums_in[8 * i : 8 * i + 8, :] + (p + q)
        total = jnp.sum(jnp.sum(s, axis=0, keepdims=True), axis=1, keepdims=True)
        out = jnp.where(lane == i, jnp.broadcast_to(total, (8, LANES)), out)
    for i in range(members // 8):
        send[8 * i : 8 * i + 8, :] = out


def fold(v):
    out = v[0:8]
    for i in range(1, v.shape[0] // 8):
        out = out + v[8 * i : 8 * i + 8]
    return out


def solve_small(t):
    g00, g10, g11, g20, g21, g22, m0, m1, m2 = t
    l1, l2 = g10 / g00, g20 / g00
    d1 = g11 - l1 * g10
    e = g21 - l2 * g10
    l3 = e / d1
    d2 = g22 - l2 * g20 - l3 * e
    y1 = m1 - l1 * m0
    y2 = m2 - l2 * m0 - l3 * y1
    c2 = y2 / d2
    c1 = y1 / d1 - l3 * c2
    return m0 / g00 - l1 * c1 - l2 * c2, c1, c2


def combine_kernel(nz, nx, *refs):
    got, b_t, u0, inside_refs, outside_refs = refs[0], refs[1], refs[2], refs[3:8], refs[8:14]
    strips, outs, staged, sems = refs[14:21], refs[21:23], refs[23:25], refs[25]
    g1i, u1i, g2i, u2i, g3i = inside_refs
    u0x, g1x, u1x, g2x, u2x, g3x = outside_refs
    every = range(nx)
    both = lambda level, i, x: Field(nz, (i, inner_rows(nx, level)), (x, outer_rows(nx, level)))
    fields = [Field(nz, (b_t, every)), Field(nz, (u0, every)), both(1, u1i, u1x), both(2, u2i, u2x)]
    fields += [both(1, g1i, g1x), both(2, g2i, g2x), both(3, g3i, g3x)]
    edges_of = [Field(nz, (ref, range(4))) for ref in strips]
    total = jnp.sum(fold(got[...]), axis=0, keepdims=True)
    line = lax.broadcasted_iota(jnp.int32, (1, LANES), 1)
    pick = lambda i: jnp.sum(jnp.where(line == i, total, 0.0), axis=1, keepdims=True)
    c0, c1, c2 = (jnp.broadcast_to(c, (8, LANES)) for c in solve_small([pick(i) for i in range(9)]))
    lane = lane_ids(8)
    inside = (lane >= STEPS) & (lane < LANES - STEPS)
    near_place = place(lane) >= STEPS

    def combined(b, v0, v1, v2, f1, f2, f3):
        return c0 * v0 + c1 * v1 + c2 * v2, b - (c0 * (b - f1) + c1 * (f1 - f2) + c2 * (f2 - f3))

    copies = []
    for block in range(nz // BLOCK):
        for k in range(block * BLOCK, (block + 1) * BLOCK, 8):
            for t in range(2):
                near, far = (combined(*(f.at(j, k) for f in edges_of)) for j in (t, t + 2))
                edges = [jnp.where(near_place, p, q) for p, q in zip(near, far)]
                for u, x, group in strip_places(nx):
                    if u != t or not t * (nx // 2) <= x < (t + 1) * (nx // 2):
                        continue
                    for ref, value, edge in zip(staged, combined(*(f.at(x, k) for f in fields)), edges):
                        turned = pltpu.roll(edge, (-(GROUP * group + STEPS)) % LANES, 1)
                        ref[pl.ds(k * nx + x, 8, stride=nx), :] = jnp.where(inside, value, turned)
        rows = pl.ds(block * BLOCK * nx, BLOCK * nx)
        for i in range(2):
            copies.append(pltpu.make_async_copy(staged[i].at[rows, :], outs[i].at[rows, :], sems.at[i, block]))
            copies[-1].start()
    for copy in copies:
        copy.wait()


def neighbours(array, axes, up):
    size = lax.axis_size(axes)
    pairs = [(i, (i + 1) % size) for i in range(size)]
    return lax.ppermute(array, axes, pairs if up else [(b, a) for a, b in pairs])


def on_device(source_heat, horiz_coef, face_coef, column_inverse):
    nz, nx, ny = source_heat.shape
    gx, gy = "gx", "gy"
    members = lax.axis_size(gx) * lax.axis_size(gy)
    part = lambda f, *a: (lambda *refs: f(*a, *refs))
    nat = source_heat.reshape(nz * nx, ny)
    low, high = pl.pallas_call(
        part(load_kernel, nz, nx),
        in_specs=[spec()],
        out_specs=[spec()] * 2,
        out_shape=[vmem(STEPS * nz)] * 2,
        compiler_params=params(4),
    )(nat)
    below = neighbours(high, gx, True)
    above = neighbours(low, gx, False)
    b_t, u0, h_wide, inner_own, outer_own, *factors = pl.pallas_call(
        part(own_kernel, nz, nx),
        in_specs=[spec()] * 3,
        out_specs=[spec()] * 8,
        out_shape=[vmem(nz * nx), vmem(nz * nx), vmem(nz), vmem(2 * nz), vmem(2 * nz)]
        + [pltpu.VMEM((nz, count * nz), BF16) for count in (3, 2, 1)],
        compiler_params=params(8),
        cost_estimate=cost(12 * nz * nz * nx * ny, 1 << 20),
    )(nat, horiz_coef.reshape(1, nz), column_inverse)
    *inside, start = pl.pallas_call(
        part(inner_kernel, nz, nx),
        in_specs=[spec()] * 6,
        out_specs=[spec()] * 6,
        out_shape=[vmem(r * nz) for r in (nx - 2, nx - 2, nx - 4, nx - 4, nx - 6)] + [vmem(72)],
        compiler_params=params(8),
        cost_estimate=cost(24 * nz * nz * nx * ny, 1 << 20),
    )(b_t, u0, h_wide, *factors)
    inner, outer = pl.pallas_call(
        part(pack_kernel, nz, nx),
        in_specs=[spec()] * 4,
        out_specs=[spec()] * 2,
        out_shape=[vmem(2 * nz)] * 2,
        compiler_params=params(4),
    )(inner_own, outer_own, below, above)
    from_left = neighbours(inner, gy, True)
    from_right = neighbours(inner, gy, False)
    *outside, sums = pl.pallas_call(
        part(outer_kernel, nz, nx),
        in_specs=[spec()] * 13,
        out_specs=[spec()] * 7,
        out_shape=[vmem(2 * STEPS * nz)] * 6 + [vmem(72)],
        compiler_params=params(8),
        cost_estimate=cost(36 * nz * nz * 6 * ny, 1 << 20),
    )(b_t, u0, below, above, h_wide, *factors, *inside[:4], start)
    *strips, send = pl.pallas_call(
        part(strip_kernel, nz, nx, members),
        in_specs=[spec()] * 9,
        out_specs=[spec()] * 8,
        out_shape=[vmem(4 * nz)] * 7 + [vmem(members)],
        compiler_params=params(8),
    )(inner, outer, from_left, from_right, h_wide, sums, *factors)
    got = lax.all_to_all(send.reshape(members, 1, LANES), (gx, gy), split_axis=0, concat_axis=0, tiled=True)
    pressure, true_residual = pl.pallas_call(
        part(combine_kernel, nz, nx),
        in_specs=[spec()] * 21,
        out_specs=[pl.BlockSpec(memory_space=pltpu.HBM)] * 2,
        out_shape=[jax.ShapeDtypeStruct((nz * nx, ny), F32)] * 2,
        scratch_shapes=[pltpu.VMEM((nz * nx, ny), F32)] * 2 + [pltpu.SemaphoreType.DMA((2, nz // BLOCK))],
        compiler_params=params(8),
    )(got.reshape(members, LANES), b_t, u0, *inside, *outside, *strips)
    return pressure.reshape(nz, nx, ny), true_residual.reshape(nz, nx, ny)


def solution(mesh):
    field = P(None, "gx", "gy")
    return jax.shard_map(
        on_device,
        mesh=mesh,
        in_specs=(field, P(), P(), P()),
        out_specs=(field, field),
        check_vma=False,
    )
```

```python
import jax
import jax.numpy as jnp
from jax import lax
from jax.experimental import pallas as pl
from jax.experimental.pallas import tpu as pltpu
from jax.sharding import Mesh
from jax.sharding import PartitionSpec as P

F32 = jnp.float32
BF16 = jnp.bfloat16
LANES = 128
GROUP = 9
STEPS = 3
WIDTH = 4
WIDE = 3
BLOCK = 32


def vmem(rows, cols=LANES):
    return pltpu.VMEM((rows, cols), F32)


def spec():
    return pl.BlockSpec(memory_space=pltpu.VMEM)


def params(mib):
    return pltpu.CompilerParams(vmem_limit_bytes=mib * 1024 * 1024)


def cost(flops, size):
    return pl.CostEstimate(flops=flops, bytes_accessed=size, transcendentals=0)


def lane_ids(rows):
    return lax.broadcasted_iota(jnp.int32, (rows, LANES), 1)


def pieces(v):
    high = v.astype(BF16)
    rest = v - high.astype(F32)
    middle = rest.astype(BF16)
    return high, middle, (rest - middle.astype(F32)).astype(BF16)


def product(factors, columns):
    nz = columns.shape[0]
    stacked = jnp.concatenate(pieces(columns), axis=0)
    dot = lambda f, count: jnp.dot(f[...], stacked[: count * nz], preferred_element_type=F32)
    return dot(factors[0], 3) + dot(factors[1], 2) + dot(factors[2], 1)


def apply_inverse(factors, src, dst, nz, tiles, width):
    for first in range(0, tiles, width):
        count = min(width, tiles - first)
        parts = [src[(first + t) * nz : (first + t + 1) * nz, :] for t in range(count)]
        out = product(factors, jnp.concatenate(parts, axis=1) if count > 1 else parts[0])
        for t in range(count):
            dst[(first + t) * nz : (first + t + 1) * nz, :] = out[:, t * LANES : (t + 1) * LANES]


def load_kernel(nz, nx, nat, low, high):
    for i in range(STEPS):
        low[i * nz : (i + 1) * nz, :] = nat[pl.ds(i, nz, stride=nx), :]
        high[i * nz : (i + 1) * nz, :] = nat[pl.ds(nx - STEPS + i, nz, stride=nx), :]


def place(lane):
    return lane - GROUP * lax.shift_right_logical(lane * 57, 9)


def strip_places(nx):
    half = nx // 2
    count = half + 2 * STEPS
    return [(t, t * half - STEPS + r, r) for t in range(2) for r in range(count)]


def add_edges(row, group, lane, inner, outer):
    first = GROUP * group
    turned = pltpu.roll(row, (first + STEPS) % LANES, 1)
    inner = jnp.where((lane >= first) & (lane < first + GROUP), turned, inner)
    if first:
        mine = (lane >= first - STEPS) & (lane < first + 2 * STEPS)
    else:
        mine = (lane >= LANES - STEPS) | (lane < 2 * STEPS)
    outer = jnp.where(mine, turned, outer)
    return inner, outer


def pack_edges(rows, first_x, nx, nz, inner, outer, tile, fresh):
    lane = lane_ids(tile)
    wanted, have = rows

    def body(i, carry):
        k = i * tile
        for t in range(2):
            at = pl.ds(pl.multiple_of(t * nz + k, 8), tile)
            if fresh:
                packed = (jnp.zeros((tile, LANES), F32),) * 2
            else:
                packed = (inner[at, :], outer[at, :])
            for u, x, group in strip_places(nx):
                if u == t and x in wanted:
                    packed = add_edges(have(x, k), group, lane, *packed)
            inner[at, :], outer[at, :] = packed
        return carry

    lax.fori_loop(0, nz // tile, body, 0, unroll=4 if fresh else True)


def own_kernel(nz, nx, nat, h_row, inv, b_t, u0, h_wide, inner, outer, *outs):
    factors, inside = outs[:3], outs[3:]
    for ref, piece, count in zip(factors, pieces(inv[...]), (3, 2, 1)):
        wide = piece.astype(F32)
        ref[...] = jnp.concatenate([wide] * count, axis=1).astype(BF16) if count > 1 else piece
    eye = lax.broadcasted_iota(jnp.int32, (nz, nz), 0) == lax.broadcasted_iota(jnp.int32, (nz, nz), 1)
    column = jnp.sum(jnp.where(eye, jnp.broadcast_to(h_row[...], (nz, nz)), 0.0), axis=1, keepdims=True)
    h_wide[...] = jnp.broadcast_to(column, (nz, LANES))
    for x in range(nx):
        b_t[x * nz : (x + 1) * nz, :] = nat[pl.ds(x, nz, stride=nx), :]
    have = lambda x, k: b_t[pl.ds(pl.multiple_of(x * nz + k, 8), 8), :]
    pack_edges((range(nx), have), 0, nx, nz, inner, outer, 8, True)
    apply_inverse(factors, b_t, u0, nz, nx, nx)
    inner_part(nz, nx, b_t, u0, h_wide, factors, *inside)


def pack_kernel(nz, nx, inner_own, outer_own, below, above, inner, outer):
    inner[...] = inner_own[...]
    outer[...] = outer_own[...]

    def have(x, k):
        ref, r = (below, x + STEPS) if x < 0 else (above, x - nx)
        return ref[pl.ds(pl.multiple_of(r * nz + k, 8), 8), :]

    wanted = [*range(-STEPS, 0), *range(nx, nx + STEPS)]
    pack_edges((wanted, have), -STEPS, nx, nz, inner, outer, 8, False)


def sideways(mid, step=1):
    return pltpu.roll(mid, step, 1) + pltpu.roll(mid, LANES - step, 1)


class Sums:
    def __init__(self):
        self.total = {}

    def add(self, terms):
        for name in terms[0]:
            row = terms[0][name]
            for more in terms[1:]:
                row = row + more[name]
            self.total[name] = row if name not in self.total else self.total[name] + row


NAMES = ("00", "10", "11", "20", "21", "22", "0b", "1b", "2b")


def stage_terms(level, b, gs, v):
    chain = (b, *gs)
    out = {f"{level}{j}": v * (chain[j] - chain[j + 1]) for j in range(level + 1)}
    out[f"{level}b"] = v * b
    return out


class Field:
    def __init__(self, nz, *places):
        self.nz = nz
        self.where = {x: (ref, i) for ref, xs in places for i, x in enumerate(xs)}

    def at(self, x, k, size=8):
        ref, i = self.where[x]
        return ref[i * self.nz + k : i * self.nz + k + size, :]


def advance(factors, xs, u_last, around, g, u, h_ref, width, visit, tile=8):
    nz = u_last.nz
    for first in range(0, len(xs), width):
        rows = []
        for i, x in enumerate(xs[first : first + width], first):
            parts, terms = [], []
            for k in range(0, nz, tile):
                parts.append(h_ref[k : k + tile, :] * around(u_last, x, k))
                found = visit(x, k, parts[-1])
                if found:
                    terms.append(found)
            visit.finish(x, terms)
            rows.append(jnp.concatenate(parts, axis=0))
            g[i * nz : (i + 1) * nz, :] = rows[-1]
        if u is None:
            continue
        out = product(factors, jnp.concatenate(rows, axis=1) if len(rows) > 1 else rows[0])
        for t in range(len(rows)):
            u[(first + t) * nz : (first + t + 1) * nz, :] = out[:, t * LANES : (t + 1) * LANES]


def five_points(v, x, k):
    return (v.at(x - 1, k) + v.at(x + 1, k)) + sideways(v.at(x, k))


def packed_points(v, x, k):
    mid = v.at(x, k)
    return sideways(mid) + sideways(mid, GROUP)


class Visit:
    def __init__(self, level, fields, mine, sums_of):
        self.level, self.fields, self.mine, self.sums_of = level, fields, mine, sums_of

    def __call__(self, x, k, g):
        if x not in self.mine:
            return None
        b, *gs, v = (field.at(x, k) for field in self.fields)
        return stage_terms(self.level, b, (*gs, g), v)

    def finish(self, x, terms):
        if terms:
            self.sums_of(x).add(terms)


def inner_rows(nx, level):
    return list(range(level, nx - level))


def outer_rows(nx, level):
    low = list(range(level - STEPS, level))
    return low + [nx - 1 - x for x in reversed(low)]


def store_sums(sums, out, start=None):
    lane = lane_ids(8)
    for i, name in enumerate(NAMES):
        at = slice(8 * i, 8 * i + 8)
        s = jnp.where((lane >= STEPS) & (lane < LANES - STEPS), sums.total[name], 0.0)
        out[at, :] = s if start is None else start[at, :] + s


def inner_part(nz, nx, b_t, u0, h_wide, factors, g1i, u1i, g2i, u2i, g3i, sums_out):
    every, sums = range(nx), Sums()
    b, v0 = Field(nz, (b_t, every)), Field(nz, (u0, every))
    rows = [inner_rows(nx, level) for level in range(STEPS + 1)]
    v1, v2 = Field(nz, (u1i, rows[1])), Field(nz, (u2i, rows[2]))
    e1, e2 = Field(nz, (g1i, rows[1])), Field(nz, (g2i, rows[2]))
    count = lambda level, *fields: Visit(level, fields, every, lambda x: sums)
    advance(factors, rows[1], v0, five_points, g1i, u1i, h_wide, WIDTH, count(0, b, v0))
    advance(factors, rows[2], v1, five_points, g2i, u2i, h_wide, WIDTH, count(1, b, e1, v1))
    advance(factors, rows[3], v2, five_points, g3i, None, h_wide, WIDTH, count(2, b, e1, e2, v2))
    store_sums(sums, sums_out)


def outer_kernel(nz, nx, b_t, u0, below, above, h_wide, f0, f1, f2, g1i, u1i, g2i, u2i, start, *outs):
    u0x, g1x, u1x, g2x, u2x, g3x, sums_out = outs
    factors, every, sums = (f0, f1, f2), range(nx), Sums()
    half = STEPS * nz
    out = product(factors, jnp.concatenate([ref[i * nz : (i + 1) * nz, :] for ref in (below, above) for i in range(STEPS)], axis=1))
    for i in range(2 * STEPS):
        u0x[i * nz : (i + 1) * nz, :] = out[:, i * LANES : (i + 1) * LANES]
    inner = [inner_rows(nx, level) for level in range(STEPS + 1)]
    outer = [outer_rows(nx, level) for level in range(STEPS + 1)]
    both = lambda level, i, x: Field(nz, (i, inner[level]), (x, outer[level]))
    b, v0, v1, v2 = Field(nz, (b_t, every)), both(0, u0, u0x), both(1, u1i, u1x), both(2, u2i, u2x)
    e1, e2 = both(1, g1i, g1x), both(2, g2i, g2x)
    count = lambda level, *fields: Visit(level, fields, every, lambda x: sums)
    advance(factors, outer[1], v0, five_points, g1x, u1x, h_wide, WIDE, count(0, b, v0))
    advance(factors, outer[2], v1, five_points, g2x, u2x, h_wide, WIDE, count(1, b, e1, v1))
    advance(factors, outer[3], v2, five_points, g3x, None, h_wide, WIDE, count(2, b, e1, e2, v2))
    store_sums(sums, sums_out, start)


def strip_kernel(nz, nx, members, inner, outer, left, right, h_wide, sums_in, f0, f1, f2, bs, u0s, u1s, u2s, g1s, g2s, g3s, send):
    factors = (f0, f1, f2)
    lane = lane_ids(nz)
    pos = place(lane)
    used = lane < GROUP * (nx // 2 + 2 * STEPS)
    for t in range(2):
        at = slice(t * nz, (t + 1) * nz)
        bs[t * nz : (t + 1) * nz, :] = jnp.where((pos < STEPS) & used, left[at, :], inner[at, :])
        bs[(t + 2) * nz : (t + 3) * nz, :] = jnp.where((pos >= STEPS) & (pos < 2 * STEPS) & used, right[at, :], outer[at, :])
    near, far, tiles = Sums(), Sums(), list(range(4))
    field = lambda ref: Field(nz, (ref, tiles))
    count = lambda level, *refs: Visit(level, [field(ref) for ref in refs], tiles, lambda j: near if j < 2 else far)
    apply_inverse(factors, bs, u0s, nz, 4, 4)
    advance(factors, tiles, field(u0s), packed_points, g1s, u1s, h_wide, 4, count(0, bs, u0s))
    advance(factors, tiles, field(u1s), packed_points, g2s, u2s, h_wide, 4, count(1, bs, g1s, u1s))
    advance(factors, tiles, field(u2s), packed_points, g3s, None, h_wide, 4, count(2, bs, g1s, g2s, u2s))
    lane = lane_ids(8)
    pos = place(lane)
    rows = (lane >= GROUP * STEPS) & (lane < GROUP * (STEPS + nx // 2))
    out = jnp.zeros((8, LANES), F32)
    for i, name in enumerate(NAMES):
        p = jnp.where(rows & (pos >= STEPS) & (pos < 2 * STEPS), near.total[name], 0.0)
        q = jnp.where(rows & (pos < STEPS), far.total[name], 0.0)
        s = sums_in[8 * i : 8 * i + 8, :] + (p + q)
        total = jnp.sum(jnp.sum(s, axis=0, keepdims=True), axis=1, keepdims=True)
        out = jnp.where(lane == i, jnp.broadcast_to(total, (8, LANES)), out)
    for i in range(members // 8):
        send[8 * i : 8 * i + 8, :] = out


def fold(v):
    out = v[0:8]
    for i in range(1, v.shape[0] // 8):
        out = out + v[8 * i : 8 * i + 8]
    return out


def solve_small(t):
    g00, g10, g11, g20, g21, g22, m0, m1, m2 = t
    l1, l2 = g10 / g00, g20 / g00
    d1 = g11 - l1 * g10
    e = g21 - l2 * g10
    l3 = e / d1
    d2 = g22 - l2 * g20 - l3 * e
    y1 = m1 - l1 * m0
    y2 = m2 - l2 * m0 - l3 * y1
    c2 = y2 / d2
    c1 = y1 / d1 - l3 * c2
    return m0 / g00 - l1 * c1 - l2 * c2, c1, c2


def combine_kernel(nz, nx, *refs):
    got, b_t, u0, inside_refs, outside_refs = refs[0], refs[1], refs[2], refs[3:8], refs[8:14]
    strips, outs, staged, sems = refs[14:21], refs[21:23], refs[23:25], refs[25]
    g1i, u1i, g2i, u2i, g3i = inside_refs
    u0x, g1x, u1x, g2x, u2x, g3x = outside_refs
    every = range(nx)
    both = lambda level, i, x: Field(nz, (i, inner_rows(nx, level)), (x, outer_rows(nx, level)))
    fields = [Field(nz, (b_t, every)), Field(nz, (u0, every)), both(1, u1i, u1x), both(2, u2i, u2x)]
    fields += [both(1, g1i, g1x), both(2, g2i, g2x), both(3, g3i, g3x)]
    edges_of = [Field(nz, (ref, range(4))) for ref in strips]
    total = jnp.sum(fold(got[...]), axis=0, keepdims=True)
    line = lax.broadcasted_iota(jnp.int32, (1, LANES), 1)
    pick = lambda i: jnp.sum(jnp.where(line == i, total, 0.0), axis=1, keepdims=True)
    c0, c1, c2 = (jnp.broadcast_to(c, (8, LANES)) for c in solve_small([pick(i) for i in range(9)]))
    lane = lane_ids(8)
    inside = (lane >= STEPS) & (lane < LANES - STEPS)
    near_place = place(lane) >= STEPS

    def combined(b, v0, v1, v2, f1, f2, f3):
        return c0 * v0 + c1 * v1 + c2 * v2, b - (c0 * (b - f1) + c1 * (f1 - f2) + c2 * (f2 - f3))

    copies = []
    for block in range(nz // BLOCK):
        for k in range(block * BLOCK, (block + 1) * BLOCK, 8):
            for t in range(2):
                near, far = (combined(*(f.at(j, k) for f in edges_of)) for j in (t, t + 2))
                edges = [jnp.where(near_place, p, q) for p, q in zip(near, far)]
                for u, x, group in strip_places(nx):
                    if u != t or not t * (nx // 2) <= x < (t + 1) * (nx // 2):
                        continue
                    for ref, value, edge in zip(staged, combined(*(f.at(x, k) for f in fields)), edges):
                        turned = pltpu.roll(edge, (-(GROUP * group + STEPS)) % LANES, 1)
                        ref[pl.ds(k * nx + x, 8, stride=nx), :] = jnp.where(inside, value, turned)
        rows = pl.ds(block * BLOCK * nx, BLOCK * nx)
        for i in range(2):
            copies.append(pltpu.make_async_copy(staged[i].at[rows, :], outs[i].at[rows, :], sems.at[i, block]))
            copies[-1].start()
    for copy in copies:
        copy.wait()


def neighbours(array, axes, up):
    size = lax.axis_size(axes)
    pairs = [(i, (i + 1) % size) for i in range(size)]
    return lax.ppermute(array, axes, pairs if up else [(b, a) for a, b in pairs])


def on_device(source_heat, horiz_coef, face_coef, column_inverse):
    nz, nx, ny = source_heat.shape
    gx, gy = "gx", "gy"
    members = lax.axis_size(gx) * lax.axis_size(gy)
    part = lambda f, *a: (lambda *refs: f(*a, *refs))
    nat = source_heat.reshape(nz * nx, ny)
    low, high = pl.pallas_call(
        part(load_kernel, nz, nx),
        in_specs=[spec()],
        out_specs=[spec()] * 2,
        out_shape=[vmem(STEPS * nz)] * 2,
        compiler_params=params(4),
    )(nat)
    below = neighbours(high, gx, True)
    above = neighbours(low, gx, False)
    b_t, u0, h_wide, inner_own, outer_own, *rest = pl.pallas_call(
        part(own_kernel, nz, nx),
        in_specs=[spec()] * 3,
        out_specs=[spec()] * 14,
        out_shape=[vmem(nz * nx), vmem(nz * nx), vmem(nz), vmem(2 * nz), vmem(2 * nz)]
        + [pltpu.VMEM((nz, count * nz), BF16) for count in (3, 2, 1)]
        + [vmem(r * nz) for r in (nx - 2, nx - 2, nx - 4, nx - 4, nx - 6)]
        + [vmem(72)],
        compiler_params=params(8),
        cost_estimate=cost(36 * nz * nz * nx * ny, 1 << 20),
    )(nat, horiz_coef.reshape(1, nz), column_inverse)
    factors, inside, start = rest[:3], rest[3:8], rest[8]
    inner, outer = pl.pallas_call(
        part(pack_kernel, nz, nx),
        in_specs=[spec()] * 4,
        out_specs=[spec()] * 2,
        out_shape=[vmem(2 * nz)] * 2,
        compiler_params=params(4),
    )(inner_own, outer_own, below, above)
    from_left = neighbours(inner, gy, True)
    from_right = neighbours(inner, gy, False)
    *outside, sums = pl.pallas_call(
        part(outer_kernel, nz, nx),
        in_specs=[spec()] * 13,
        out_specs=[spec()] * 7,
        out_shape=[vmem(2 * STEPS * nz)] * 6 + [vmem(72)],
        compiler_params=params(8),
        cost_estimate=cost(36 * nz * nz * 6 * ny, 1 << 20),
    )(b_t, u0, below, above, h_wide, *factors, *inside[:4], start)
    *strips, send = pl.pallas_call(
        part(strip_kernel, nz, nx, members),
        in_specs=[spec()] * 9,
        out_specs=[spec()] * 8,
        out_shape=[vmem(4 * nz)] * 7 + [vmem(members)],
        compiler_params=params(8),
    )(inner, outer, from_left, from_right, h_wide, sums, *factors)
    got = lax.all_to_all(send.reshape(members, 1, LANES), (gx, gy), split_axis=0, concat_axis=0, tiled=True)
    pressure, true_residual = pl.pallas_call(
        part(combine_kernel, nz, nx),
        in_specs=[spec()] * 21,
        out_specs=[pl.BlockSpec(memory_space=pltpu.HBM)] * 2,
        out_shape=[jax.ShapeDtypeStruct((nz * nx, ny), F32)] * 2,
        scratch_shapes=[pltpu.VMEM((nz * nx, ny), F32)] * 2 + [pltpu.SemaphoreType.DMA((2, nz // BLOCK))],
        compiler_params=params(8),
    )(got.reshape(members, LANES), b_t, u0, *inside, *outside, *strips)
    return pressure.reshape(nz, nx, ny), true_residual.reshape(nz, nx, ny)


def solution(mesh):
    field = P(None, "gx", "gy")
    return jax.shard_map(
        on_device,
        mesh=mesh,
        in_specs=(field, P(), P(), P()),
        out_specs=(field, field),
        check_vma=False,
    )
```

```python
import jax
import jax.numpy as jnp
from jax import lax
from jax.experimental import pallas as pl
from jax.experimental.pallas import tpu as pltpu
from jax.sharding import PartitionSpec as P

F32 = jnp.float32
BF16 = jnp.bfloat16
LANES = 128
GROUP = 9
STEPS = 3
WIDTH = 4
WIDE = 3
BLOCK = 32


def vmem(rows, cols=LANES):
    return pltpu.VMEM((rows, cols), F32)


def spec():
    return pl.BlockSpec(memory_space=pltpu.VMEM)


def params(mib):
    return pltpu.CompilerParams(vmem_limit_bytes=mib * 1024 * 1024)


def cost(flops, size):
    return pl.CostEstimate(flops=flops, bytes_accessed=size, transcendentals=0)


def lane_ids(rows):
    return lax.broadcasted_iota(jnp.int32, (rows, LANES), 1)


def pieces(v):
    high = v.astype(BF16)
    rest = v - high.astype(F32)
    middle = rest.astype(BF16)
    return high, middle, (rest - middle.astype(F32)).astype(BF16)


def product(factors, columns):
    nz = columns.shape[0]
    stacked = jnp.concatenate(pieces(columns), axis=0)
    dot = lambda f, count: jnp.dot(f[...], stacked[: count * nz], preferred_element_type=F32)
    return dot(factors[0], 3) + dot(factors[1], 2) + dot(factors[2], 1)


def apply_inverse(factors, src, dst, nz, tiles, width):
    for first in range(0, tiles, width):
        count = min(width, tiles - first)
        parts = [src[(first + t) * nz : (first + t + 1) * nz, :] for t in range(count)]
        out = product(factors, jnp.concatenate(parts, axis=1) if count > 1 else parts[0])
        for t in range(count):
            dst[(first + t) * nz : (first + t + 1) * nz, :] = out[:, t * LANES : (t + 1) * LANES]


def load_kernel(nz, nx, nat, low, high, far_low, far_high):
    for i in range(2):
        low[i * nz : (i + 1) * nz, :] = nat[pl.ds(i, nz, stride=nx), :]
        high[i * nz : (i + 1) * nz, :] = nat[pl.ds(nx - 2 + i, nz, stride=nx), :]
    far_low[...] = nat[pl.ds(2, nz, stride=nx), :]
    far_high[...] = nat[pl.ds(nx - STEPS, nz, stride=nx), :]


def place(lane):
    return lane - GROUP * lax.shift_right_logical(lane * 57, 9)


def strip_places(nx):
    half = nx // 2
    count = half + 2 * STEPS
    return [(t, t * half - STEPS + r, r) for t in range(2) for r in range(count)]


def add_edges(row, group, lane, inner, outer):
    first = GROUP * group
    turned = pltpu.roll(row, (first + STEPS) % LANES, 1)
    inner = jnp.where((lane >= first) & (lane < first + GROUP), turned, inner)
    if first:
        mine = (lane >= first - STEPS) & (lane < first + 2 * STEPS)
    else:
        mine = (lane >= LANES - STEPS) | (lane < 2 * STEPS)
    outer = jnp.where(mine, turned, outer)
    return inner, outer


def pack_edges(rows, nx, nz, inner, outer, tile, fresh):
    lane = lane_ids(tile)
    wanted, have = rows

    def body(i, carry):
        k = i * tile
        for t in range(2):
            at = pl.ds(pl.multiple_of(t * nz + k, 8), tile)
            if fresh:
                packed = (jnp.zeros((tile, LANES), F32),) * 2
            else:
                packed = (inner[at, :], outer[at, :])
            for u, x, group in strip_places(nx):
                if u == t and x in wanted:
                    packed = add_edges(have(x, k), group, lane, *packed)
            inner[at, :], outer[at, :] = packed
        return carry

    lax.fori_loop(0, nz // tile, body, 0, unroll=4 if fresh else True)


def own_kernel(nz, nx, nat, h_row, inv, b_t, u0, h_wide, inner, outer, *outs):
    factors, inside = outs[:3], outs[3:]
    for ref, piece, count in zip(factors, pieces(inv[...]), (3, 2, 1)):
        wide = piece.astype(F32)
        ref[...] = jnp.concatenate([wide] * count, axis=1).astype(BF16) if count > 1 else piece
    eye = lax.broadcasted_iota(jnp.int32, (nz, nz), 0) == lax.broadcasted_iota(jnp.int32, (nz, nz), 1)
    column = jnp.sum(jnp.where(eye, jnp.broadcast_to(h_row[...], (nz, nz)), 0.0), axis=1, keepdims=True)
    h_wide[...] = jnp.broadcast_to(column, (nz, LANES))
    for x in range(nx):
        b_t[x * nz : (x + 1) * nz, :] = nat[pl.ds(x, nz, stride=nx), :]
    have = lambda x, k: b_t[pl.ds(pl.multiple_of(x * nz + k, 8), 8), :]
    pack_edges((range(nx), have), nx, nz, inner, outer, 8, True)
    apply_inverse(factors, b_t, u0, nz, nx, nx)
    inner_part(nz, nx, b_t, u0, h_wide, factors, *inside)


def pack_kernel(nz, nx, inner_own, outer_own, below, above, inner, outer, to_right, to_left):
    inner[...] = inner_own[...]
    outer[...] = outer_own[...]
    halo = Field(nz, (below, (-2, -1)), (above, (nx, nx + 1)))
    rows = (list(halo.where), lambda x, k: halo.ref_at(x, k))
    pack_edges(rows, nx, nz, inner, outer, 8, False)
    pos = place(lane_ids(nz))
    first, second = inner[:nz, :], pltpu.roll(inner[nz:, :], STEPS, 1)
    to_right[...] = jnp.where(pos < STEPS, first, second)
    to_left[...] = jnp.where(pos < 2 * STEPS, first, second)


def sideways(mid, step=1):
    return pltpu.roll(mid, step, 1) + pltpu.roll(mid, LANES - step, 1)


class Sums:
    def __init__(self):
        self.total = {}

    def add(self, terms):
        for name in terms[0]:
            row = terms[0][name]
            for more in terms[1:]:
                row = row + more[name]
            self.total[name] = row if name not in self.total else self.total[name] + row


NAMES = ("00", "10", "11", "20", "21", "22", "0b", "1b", "2b")


def stage_terms(level, b, gs, v):
    chain = (b, *gs)
    out = {f"{level}{j}": v * (chain[j] - chain[j + 1]) for j in range(level + 1)}
    out[f"{level}b"] = v * b
    return out


class Field:
    def __init__(self, nz, *places):
        self.nz = nz
        self.where = {x: (ref, i) for ref, xs in places for i, x in enumerate(xs)}

    def at(self, x, k, size=8):
        ref, i = self.where[x]
        return ref[i * self.nz + k : i * self.nz + k + size, :]

    def ref_at(self, x, k, size=8):
        ref, i = self.where[x]
        return ref[pl.ds(pl.multiple_of(i * self.nz + k, 8), size), :]


def advance(factors, xs, u_last, around, g, u, h_ref, width, visit, tile=8):
    nz = u_last.nz
    for first in range(0, len(xs), width):
        rows = []
        for i, x in enumerate(xs[first : first + width], first):
            parts, terms = [], []
            for k in range(0, nz, tile):
                parts.append(h_ref[k : k + tile, :] * around(u_last, x, k))
                found = visit(x, k, parts[-1])
                if found:
                    terms.append(found)
            visit.finish(x, terms)
            rows.append(jnp.concatenate(parts, axis=0))
            g[i * nz : (i + 1) * nz, :] = rows[-1]
        if u is None:
            continue
        out = product(factors, jnp.concatenate(rows, axis=1) if len(rows) > 1 else rows[0])
        for t in range(len(rows)):
            u[(first + t) * nz : (first + t + 1) * nz, :] = out[:, t * LANES : (t + 1) * LANES]


def five_points(v, x, k):
    return (v.at(x - 1, k) + v.at(x + 1, k)) + sideways(v.at(x, k))


def packed_points(v, x, k):
    mid = v.at(x, k)
    return sideways(mid) + sideways(mid, GROUP)


class Visit:
    def __init__(self, level, fields, mine, sums_of):
        self.level, self.fields, self.mine, self.sums_of = level, fields, mine, sums_of

    def __call__(self, x, k, g):
        if x not in self.mine:
            return None
        b, *gs, v = (field.at(x, k) for field in self.fields)
        return stage_terms(self.level, b, (*gs, g), v)

    def finish(self, x, terms):
        if terms:
            self.sums_of(x).add(terms)


def inner_rows(nx, level):
    return list(range(level, nx - level))


def outer_rows(nx, level):
    low = list(range(level - STEPS, level))
    return low + [nx - 1 - x for x in reversed(low)]


def store_sums(sums, out, start=None):
    lane = lane_ids(8)
    for i, name in enumerate(NAMES):
        at = slice(8 * i, 8 * i + 8)
        s = jnp.where((lane >= STEPS) & (lane < LANES - STEPS), sums.total[name], 0.0)
        out[at, :] = s if start is None else start[at, :] + s


def inner_part(nz, nx, b_t, u0, h_wide, factors, g1i, u1i, g2i, u2i, g3i, sums_out):
    every, sums = range(nx), Sums()
    b, v0 = Field(nz, (b_t, every)), Field(nz, (u0, every))
    rows = [inner_rows(nx, level) for level in range(STEPS + 1)]
    v1, v2 = Field(nz, (u1i, rows[1])), Field(nz, (u2i, rows[2]))
    e1, e2 = Field(nz, (g1i, rows[1])), Field(nz, (g2i, rows[2]))
    count = lambda level, *fields: Visit(level, fields, every, lambda x: sums)
    advance(factors, rows[1], v0, five_points, g1i, u1i, h_wide, WIDTH, count(0, b, v0))
    advance(factors, rows[2], v1, five_points, g2i, u2i, h_wide, WIDTH, count(1, b, e1, v1))
    advance(factors, rows[3], v2, five_points, g3i, None, h_wide, WIDTH, count(2, b, e1, e2, v2))
    store_sums(sums, sums_out)


def outer_kernel(nz, nx, b_t, u0, below, above, far_below, far_above, edges_in, edges_out, h_wide, f0, f1, f2, *refs):
    g1i, u1i, g2i, u2i, start, u0x, g1x, u1x, g2x, u2x, g3x, sums_out, edges_in_all, edges_out_all = refs
    factors, every, sums = (f0, f1, f2), range(nx), Sums()
    halo = Field(nz, (far_below, (-3,)), (below, (-2, -1)), (above, (nx, nx + 1)), (far_above, (nx + 2,)))
    out = product(factors, jnp.concatenate([halo.at(x, 0, nz) for x in outer_rows(nx, 0)], axis=1))
    for i in range(2 * STEPS):
        u0x[i * nz : (i + 1) * nz, :] = out[:, i * LANES : (i + 1) * LANES]
    edges_in_all[...] = edges_in[...]
    edges_out_all[...] = edges_out[...]
    rows = ((-STEPS, nx + STEPS - 1), lambda x, k: halo.ref_at(x, k))
    pack_edges(rows, nx, nz, edges_in_all, edges_out_all, 8, False)
    inner = [inner_rows(nx, level) for level in range(STEPS + 1)]
    outer = [outer_rows(nx, level) for level in range(STEPS + 1)]
    both = lambda level, i, x: Field(nz, (i, inner[level]), (x, outer[level]))
    b, v0, v1, v2 = Field(nz, (b_t, every)), both(0, u0, u0x), both(1, u1i, u1x), both(2, u2i, u2x)
    e1, e2 = both(1, g1i, g1x), both(2, g2i, g2x)
    count = lambda level, *fields: Visit(level, fields, every, lambda x: sums)
    advance(factors, outer[1], v0, five_points, g1x, u1x, h_wide, WIDE, count(0, b, v0))
    advance(factors, outer[2], v1, five_points, g2x, u2x, h_wide, WIDE, count(1, b, e1, v1))
    advance(factors, outer[3], v2, five_points, g3x, None, h_wide, WIDE, count(2, b, e1, e2, v2))
    store_sums(sums, sums_out, start)


def strip_kernel(nz, nx, members, inner, outer, left, right, h_wide, sums_in, f0, f1, f2, bs, u0s, u1s, u2s, g1s, g2s, g3s, send):
    factors = (f0, f1, f2)
    lane = lane_ids(nz)
    pos = place(lane)
    used = lane < GROUP * (nx // 2 + 2 * STEPS)
    for t in range(2):
        at = slice(t * nz, (t + 1) * nz)
        beyond = [pltpu.roll(ref[...], LANES - STEPS, 1) if t else ref[...] for ref in (left, right)]
        bs[t * nz : (t + 1) * nz, :] = jnp.where((pos < STEPS) & used, beyond[0], inner[at, :])
        bs[(t + 2) * nz : (t + 3) * nz, :] = jnp.where((pos >= STEPS) & (pos < 2 * STEPS) & used, beyond[1], outer[at, :])
    near, far, tiles = Sums(), Sums(), list(range(4))
    field = lambda ref: Field(nz, (ref, tiles))
    count = lambda level, *refs: Visit(level, [field(ref) for ref in refs], tiles, lambda j: near if j < 2 else far)
    apply_inverse(factors, bs, u0s, nz, 4, 4)
    advance(factors, tiles, field(u0s), packed_points, g1s, u1s, h_wide, 4, count(0, bs, u0s))
    advance(factors, tiles, field(u1s), packed_points, g2s, u2s, h_wide, 4, count(1, bs, g1s, u1s))
    advance(factors, tiles, field(u2s), packed_points, g3s, None, h_wide, 4, count(2, bs, g1s, g2s, u2s))
    lane = lane_ids(8)
    pos = place(lane)
    rows = (lane >= GROUP * STEPS) & (lane < GROUP * (STEPS + nx // 2))
    out = jnp.zeros((8, LANES), F32)
    for i, name in enumerate(NAMES):
        p = jnp.where(rows & (pos >= STEPS) & (pos < 2 * STEPS), near.total[name], 0.0)
        q = jnp.where(rows & (pos < STEPS), far.total[name], 0.0)
        s = sums_in[8 * i : 8 * i + 8, :] + (p + q)
        total = jnp.sum(jnp.sum(s, axis=0, keepdims=True), axis=1, keepdims=True)
        out = jnp.where(lane == i, jnp.broadcast_to(total, (8, LANES)), out)
    for i in range(members // 8):
        send[8 * i : 8 * i + 8, :] = out


def fold(v):
    out = v[0:8]
    for i in range(1, v.shape[0] // 8):
        out = out + v[8 * i : 8 * i + 8]
    return out


def solve_small(t):
    g00, g10, g11, g20, g21, g22, m0, m1, m2 = t
    l1, l2 = g10 / g00, g20 / g00
    d1 = g11 - l1 * g10
    e = g21 - l2 * g10
    l3 = e / d1
    d2 = g22 - l2 * g20 - l3 * e
    y1 = m1 - l1 * m0
    y2 = m2 - l2 * m0 - l3 * y1
    c2 = y2 / d2
    c1 = y1 / d1 - l3 * c2
    return m0 / g00 - l1 * c1 - l2 * c2, c1, c2


def combine_kernel(nz, nx, *refs):
    got, b_t, u0, inside_refs, outside_refs = refs[0], refs[1], refs[2], refs[3:8], refs[8:14]
    strips, outs, staged, sems = refs[14:21], refs[21:23], refs[23:25], refs[25]
    g1i, u1i, g2i, u2i, g3i = inside_refs
    _, g1x, u1x, g2x, u2x, g3x = outside_refs
    every = range(nx)
    both = lambda level, i, x: Field(nz, (i, inner_rows(nx, level)), (x, outer_rows(nx, level)))
    fields = [Field(nz, (b_t, every)), Field(nz, (u0, every)), both(1, u1i, u1x), both(2, u2i, u2x)]
    fields += [both(1, g1i, g1x), both(2, g2i, g2x), both(3, g3i, g3x)]
    edges_of = [Field(nz, (ref, range(4))) for ref in strips]
    total = jnp.sum(fold(got[...]), axis=0, keepdims=True)
    line = lax.broadcasted_iota(jnp.int32, (1, LANES), 1)
    pick = lambda i: jnp.sum(jnp.where(line == i, total, 0.0), axis=1, keepdims=True)
    c0, c1, c2 = (jnp.broadcast_to(c, (8, LANES)) for c in solve_small([pick(i) for i in range(9)]))
    lane = lane_ids(8)
    inside = (lane >= STEPS) & (lane < LANES - STEPS)
    near_place = place(lane) >= STEPS

    def combined(b, v0, v1, v2, f1, f2, f3):
        return c0 * v0 + c1 * v1 + c2 * v2, b - (c0 * (b - f1) + c1 * (f1 - f2) + c2 * (f2 - f3))

    copies = []
    for block in range(nz // BLOCK):
        for k in range(block * BLOCK, (block + 1) * BLOCK, 8):
            for t in range(2):
                near, far = (combined(*(f.at(j, k) for f in edges_of)) for j in (t, t + 2))
                edges = [jnp.where(near_place, p, q) for p, q in zip(near, far)]
                for u, x, group in strip_places(nx):
                    if u != t or not t * (nx // 2) <= x < (t + 1) * (nx // 2):
                        continue
                    for ref, value, edge in zip(staged, combined(*(f.at(x, k) for f in fields)), edges):
                        turned = pltpu.roll(edge, (-(GROUP * group + STEPS)) % LANES, 1)
                        ref[pl.ds(k * nx + x, 8, stride=nx), :] = jnp.where(inside, value, turned)
        rows = pl.ds(block * BLOCK * nx, BLOCK * nx)
        for i in range(2):
            copies.append(pltpu.make_async_copy(staged[i].at[rows, :], outs[i].at[rows, :], sems.at[i, block]))
            copies[-1].start()
    for copy in copies:
        copy.wait()


def neighbours(array, axes, up):
    size = lax.axis_size(axes)
    pairs = [(i, (i + 1) % size) for i in range(size)]
    return lax.ppermute(array, axes, pairs if up else [(b, a) for a, b in pairs])


def on_device(source_heat, horiz_coef, face_coef, column_inverse):
    nz, nx, ny = source_heat.shape
    gx, gy = "gx", "gy"
    members = lax.axis_size(gx) * lax.axis_size(gy)
    part = lambda f, *a: (lambda *refs: f(*a, *refs))
    nat = source_heat.reshape(nz * nx, ny)
    low, high, far_low, far_high = pl.pallas_call(
        part(load_kernel, nz, nx),
        in_specs=[spec()],
        out_specs=[spec()] * 4,
        out_shape=[vmem(2 * nz)] * 2 + [vmem(nz)] * 2,
        compiler_params=params(4),
    )(nat)
    below = neighbours(high, gx, True)
    above = neighbours(low, gx, False)
    far_below = neighbours(far_high, gx, True)
    far_above = neighbours(far_low, gx, False)
    b_t, u0, h_wide, inner_own, outer_own, *rest = pl.pallas_call(
        part(own_kernel, nz, nx),
        in_specs=[spec()] * 3,
        out_specs=[spec()] * 14,
        out_shape=[vmem(nz * nx), vmem(nz * nx), vmem(nz), vmem(2 * nz), vmem(2 * nz)]
        + [pltpu.VMEM((nz, count * nz), BF16) for count in (3, 2, 1)]
        + [vmem(r * nz) for r in (nx - 2, nx - 2, nx - 4, nx - 4, nx - 6)]
        + [vmem(72)],
        compiler_params=params(8),
        cost_estimate=cost(36 * nz * nz * nx * ny, 1 << 20),
    )(nat, horiz_coef.reshape(1, nz), column_inverse)
    factors, inside, start = rest[:3], rest[3:8], rest[8]
    inner, outer, to_right, to_left = pl.pallas_call(
        part(pack_kernel, nz, nx),
        in_specs=[spec()] * 4,
        out_specs=[spec()] * 4,
        out_shape=[vmem(2 * nz)] * 2 + [vmem(nz)] * 2,
        compiler_params=params(4),
    )(inner_own, outer_own, below, above)
    from_left = neighbours(to_right, gy, True)
    from_right = neighbours(to_left, gy, False)
    *outside, sums, inner, outer = pl.pallas_call(
        part(outer_kernel, nz, nx),
        in_specs=[spec()] * 17,
        out_specs=[spec()] * 9,
        out_shape=[vmem(2 * STEPS * nz)] * 6 + [vmem(72)] + [vmem(2 * nz)] * 2,
        compiler_params=params(8),
        cost_estimate=cost(36 * nz * nz * 6 * ny, 1 << 20),
    )(b_t, u0, below, above, far_below, far_above, inner, outer, h_wide, *factors, *inside[:4], start)
    *strips, send = pl.pallas_call(
        part(strip_kernel, nz, nx, members),
        in_specs=[spec()] * 9,
        out_specs=[spec()] * 8,
        out_shape=[vmem(4 * nz)] * 7 + [vmem(members)],
        compiler_params=params(8),
    )(inner, outer, from_left, from_right, h_wide, sums, *factors)
    got = lax.all_to_all(send.reshape(members, 1, LANES), (gx, gy), split_axis=0, concat_axis=0, tiled=True)
    pressure, true_residual = pl.pallas_call(
        part(combine_kernel, nz, nx),
        in_specs=[spec()] * 21,
        out_specs=[pl.BlockSpec(memory_space=pltpu.HBM)] * 2,
        out_shape=[jax.ShapeDtypeStruct((nz * nx, ny), F32)] * 2,
        scratch_shapes=[pltpu.VMEM((nz * nx, ny), F32)] * 2 + [pltpu.SemaphoreType.DMA((2, nz // BLOCK))],
        compiler_params=params(8),
    )(got.reshape(members, LANES), b_t, u0, *inside, *outside, *strips)
    return pressure.reshape(nz, nx, ny), true_residual.reshape(nz, nx, ny)


def solution(mesh):
    field = P(None, "gx", "gy")
    return jax.shard_map(
        on_device,
        mesh=mesh,
        in_specs=(field, P(), P(), P()),
        out_specs=(field, field),
        check_vma=False,
    )
```

```python
import jax
import jax.numpy as jnp
from jax import lax
from jax.experimental import pallas as pl
from jax.experimental.pallas import tpu as pltpu
from jax.sharding import Mesh
from jax.sharding import PartitionSpec as P

F32 = jnp.float32
BF16 = jnp.bfloat16
LANES = 128
GROUP = 9
STEPS = 3
WIDTH = 4
WIDE = 3
BLOCK = 32


def vmem(rows, cols=LANES):
    return pltpu.VMEM((rows, cols), F32)


def spec():
    return pl.BlockSpec(memory_space=pltpu.VMEM)


def params(mib):
    return pltpu.CompilerParams(vmem_limit_bytes=mib * 1024 * 1024)


def cost(flops, size):
    return pl.CostEstimate(flops=flops, bytes_accessed=size, transcendentals=0)


def lane_ids(rows):
    return lax.broadcasted_iota(jnp.int32, (rows, LANES), 1)


def pieces(v):
    high = v.astype(BF16)
    rest = v - high.astype(F32)
    middle = rest.astype(BF16)
    return high, middle, (rest - middle.astype(F32)).astype(BF16)


def product(factors, columns):
    nz = columns.shape[0]
    stacked = jnp.concatenate(pieces(columns), axis=0)
    dot = lambda f, count: jnp.dot(f[...], stacked[: count * nz], preferred_element_type=F32)
    return dot(factors[0], 3) + dot(factors[1], 2) + dot(factors[2], 1)


def apply_inverse(factors, src, dst, nz, tiles, width):
    for first in range(0, tiles, width):
        count = min(width, tiles - first)
        parts = [src[(first + t) * nz : (first + t + 1) * nz, :] for t in range(count)]
        out = product(factors, jnp.concatenate(parts, axis=1) if count > 1 else parts[0])
        for t in range(count):
            dst[(first + t) * nz : (first + t + 1) * nz, :] = out[:, t * LANES : (t + 1) * LANES]


def load_kernel(nz, nx, nat, low, high):
    for i in range(STEPS):
        low[i * nz : (i + 1) * nz, :] = nat[pl.ds(i, nz, stride=nx), :]
        high[i * nz : (i + 1) * nz, :] = nat[pl.ds(nx - STEPS + i, nz, stride=nx), :]


def place(lane):
    return lane - GROUP * lax.shift_right_logical(lane * 57, 9)


def strip_places(nx):
    half = nx // 2
    count = half + 2 * STEPS
    return [(t, t * half - STEPS + r, r) for t in range(2) for r in range(count)]


def add_edges(row, group, lane, inner, outer):
    first = GROUP * group
    turned = pltpu.roll(row, (first + STEPS) % LANES, 1)
    inner = jnp.where((lane >= first) & (lane < first + GROUP), turned, inner)
    if first:
        mine = (lane >= first - STEPS) & (lane < first + 2 * STEPS)
    else:
        mine = (lane >= LANES - STEPS) | (lane < 2 * STEPS)
    outer = jnp.where(mine, turned, outer)
    return inner, outer


def pack_edges(rows, first_x, nx, nz, inner, outer, tile, fresh):
    lane = lane_ids(tile)
    wanted, have = rows

    def body(i, carry):
        k = i * tile
        for t in range(2):
            at = pl.ds(pl.multiple_of(t * nz + k, 8), tile)
            if fresh:
                packed = (jnp.zeros((tile, LANES), F32),) * 2
            else:
                packed = (inner[at, :], outer[at, :])
            for u, x, group in strip_places(nx):
                if u == t and x in wanted:
                    packed = add_edges(have(x, k), group, lane, *packed)
            inner[at, :], outer[at, :] = packed
        return carry

    lax.fori_loop(0, nz // tile, body, 0, unroll=4 if fresh else True)


def own_kernel(nz, nx, nat, h_row, inv, b_t, u0, h_wide, inner, outer, *outs):
    factors, inside = outs[:3], outs[3:]
    for ref, piece, count in zip(factors, pieces(inv[...]), (3, 2, 1)):
        wide = piece.astype(F32)
        ref[...] = jnp.concatenate([wide] * count, axis=1).astype(BF16) if count > 1 else piece
    eye = lax.broadcasted_iota(jnp.int32, (nz, nz), 0) == lax.broadcasted_iota(jnp.int32, (nz, nz), 1)
    column = jnp.sum(jnp.where(eye, jnp.broadcast_to(h_row[...], (nz, nz)), 0.0), axis=1, keepdims=True)
    h_wide[...] = jnp.broadcast_to(column, (nz, LANES))
    for x in range(nx):
        b_t[x * nz : (x + 1) * nz, :] = nat[pl.ds(x, nz, stride=nx), :]
    have = lambda x, k: b_t[pl.ds(pl.multiple_of(x * nz + k, 8), 8), :]
    pack_edges((range(nx), have), 0, nx, nz, inner, outer, 8, True)
    apply_inverse(factors, b_t, u0, nz, nx, nx)
    inner_part(nz, nx, b_t, u0, h_wide, factors, *inside)


def pack_kernel(nz, nx, inner_own, outer_own, below, above, inner, outer, to_right, to_left):
    inner[...] = inner_own[...]
    outer[...] = outer_own[...]

    def have(x, k):
        ref, r = (below, x + STEPS) if x < 0 else (above, x - nx)
        return ref[pl.ds(pl.multiple_of(r * nz + k, 8), 8), :]

    wanted = [*range(-STEPS, 0), *range(nx, nx + STEPS)]
    pack_edges((wanted, have), -STEPS, nx, nz, inner, outer, 8, False)
    pos = place(lane_ids(nz))
    first, second = inner[:nz, :], pltpu.roll(inner[nz:, :], STEPS, 1)
    to_right[...] = jnp.where(pos < STEPS, first, second)
    to_left[...] = jnp.where(pos < 2 * STEPS, first, second)


def sideways(mid, step=1):
    return pltpu.roll(mid, step, 1) + pltpu.roll(mid, LANES - step, 1)


class Sums:
    def __init__(self):
        self.total = {}

    def add(self, terms):
        for name in terms[0]:
            row = terms[0][name]
            for more in terms[1:]:
                row = row + more[name]
            self.total[name] = row if name not in self.total else self.total[name] + row


NAMES = ("00", "10", "11", "20", "21", "22", "0b", "1b", "2b")


def stage_terms(level, b, gs, v):
    chain = (b, *gs)
    out = {f"{level}{j}": v * (chain[j] - chain[j + 1]) for j in range(level + 1)}
    out[f"{level}b"] = v * b
    return out


class Field:
    def __init__(self, nz, *places):
        self.nz = nz
        self.where = {x: (ref, i) for ref, xs in places for i, x in enumerate(xs)}

    def at(self, x, k, size=8):
        ref, i = self.where[x]
        return ref[i * self.nz + k : i * self.nz + k + size, :]


def advance(factors, xs, u_last, around, g, u, h_ref, width, visit, tile=8):
    nz = u_last.nz
    for first in range(0, len(xs), width):
        rows = []
        for i, x in enumerate(xs[first : first + width], first):
            parts, terms = [], []
            for k in range(0, nz, tile):
                parts.append(h_ref[k : k + tile, :] * around(u_last, x, k))
                found = visit(x, k, parts[-1])
                if found:
                    terms.append(found)
            visit.finish(x, terms)
            rows.append(jnp.concatenate(parts, axis=0))
            g[i * nz : (i + 1) * nz, :] = rows[-1]
        if u is None:
            continue
        out = product(factors, jnp.concatenate(rows, axis=1) if len(rows) > 1 else rows[0])
        for t in range(len(rows)):
            u[(first + t) * nz : (first + t + 1) * nz, :] = out[:, t * LANES : (t + 1) * LANES]


def five_points(v, x, k):
    return (v.at(x - 1, k) + v.at(x + 1, k)) + sideways(v.at(x, k))


def packed_points(v, x, k):
    mid = v.at(x, k)
    return sideways(mid) + sideways(mid, GROUP)


class Visit:
    def __init__(self, level, fields, mine, sums_of):
        self.level, self.fields, self.mine, self.sums_of = level, fields, mine, sums_of

    def __call__(self, x, k, g):
        if x not in self.mine:
            return None
        b, *gs, v = (field.at(x, k) for field in self.fields)
        return stage_terms(self.level, b, (*gs, g), v)

    def finish(self, x, terms):
        if terms:
            self.sums_of(x).add(terms)


def inner_rows(nx, level):
    return list(range(level, nx - level))


def outer_rows(nx, level):
    low = list(range(level - STEPS, level))
    return low + [nx - 1 - x for x in reversed(low)]


def store_sums(sums, out, start=None):
    lane = lane_ids(8)
    for i, name in enumerate(NAMES):
        at = slice(8 * i, 8 * i + 8)
        s = jnp.where((lane >= STEPS) & (lane < LANES - STEPS), sums.total[name], 0.0)
        out[at, :] = s if start is None else start[at, :] + s


def inner_part(nz, nx, b_t, u0, h_wide, factors, g1i, u1i, g2i, u2i, g3i, sums_out):
    every, sums = range(nx), Sums()
    b, v0 = Field(nz, (b_t, every)), Field(nz, (u0, every))
    rows = [inner_rows(nx, level) for level in range(STEPS + 1)]
    v1, v2 = Field(nz, (u1i, rows[1])), Field(nz, (u2i, rows[2]))
    e1, e2 = Field(nz, (g1i, rows[1])), Field(nz, (g2i, rows[2]))
    count = lambda level, *fields: Visit(level, fields, every, lambda x: sums)
    advance(factors, rows[1], v0, five_points, g1i, u1i, h_wide, WIDTH, count(0, b, v0))
    advance(factors, rows[2], v1, five_points, g2i, u2i, h_wide, WIDTH, count(1, b, e1, v1))
    advance(factors, rows[3], v2, five_points, g3i, None, h_wide, WIDTH, count(2, b, e1, e2, v2))
    store_sums(sums, sums_out)


def outer_kernel(nz, nx, b_t, u0, below, above, h_wide, f0, f1, f2, g1i, u1i, g2i, u2i, start, *outs):
    u0x, g1x, u1x, g2x, u2x, g3x, sums_out = outs
    factors, every, sums = (f0, f1, f2), range(nx), Sums()
    half = STEPS * nz
    out = product(factors, jnp.concatenate([ref[i * nz : (i + 1) * nz, :] for ref in (below, above) for i in range(STEPS)], axis=1))
    for i in range(2 * STEPS):
        u0x[i * nz : (i + 1) * nz, :] = out[:, i * LANES : (i + 1) * LANES]
    inner = [inner_rows(nx, level) for level in range(STEPS + 1)]
    outer = [outer_rows(nx, level) for level in range(STEPS + 1)]
    both = lambda level, i, x: Field(nz, (i, inner[level]), (x, outer[level]))
    b, v0, v1, v2 = Field(nz, (b_t, every)), both(0, u0, u0x), both(1, u1i, u1x), both(2, u2i, u2x)
    e1, e2 = both(1, g1i, g1x), both(2, g2i, g2x)
    count = lambda level, *fields: Visit(level, fields, every, lambda x: sums)
    advance(factors, outer[1], v0, five_points, g1x, u1x, h_wide, WIDE, count(0, b, v0))
    advance(factors, outer[2], v1, five_points, g2x, u2x, h_wide, WIDE, count(1, b, e1, v1))
    advance(factors, outer[3], v2, five_points, g3x, None, h_wide, WIDE, count(2, b, e1, e2, v2))
    store_sums(sums, sums_out, start)


def strip_kernel(nz, nx, members, inner, outer, left, right, h_wide, sums_in, f0, f1, f2, bs, u0s, u1s, u2s, g1s, g2s, g3s, send):
    factors = (f0, f1, f2)
    lane = lane_ids(nz)
    pos = place(lane)
    used = lane < GROUP * (nx // 2 + 2 * STEPS)
    for t in range(2):
        at = slice(t * nz, (t + 1) * nz)
        beyond = [pltpu.roll(ref[...], LANES - STEPS, 1) if t else ref[...] for ref in (left, right)]
        bs[t * nz : (t + 1) * nz, :] = jnp.where((pos < STEPS) & used, beyond[0], inner[at, :])
        bs[(t + 2) * nz : (t + 3) * nz, :] = jnp.where((pos >= STEPS) & (pos < 2 * STEPS) & used, beyond[1], outer[at, :])
    near, far, tiles = Sums(), Sums(), list(range(4))
    field = lambda ref: Field(nz, (ref, tiles))
    count = lambda level, *refs: Visit(level, [field(ref) for ref in refs], tiles, lambda j: near if j < 2 else far)
    apply_inverse(factors, bs, u0s, nz, 4, 4)
    advance(factors, tiles, field(u0s), packed_points, g1s, u1s, h_wide, 4, count(0, bs, u0s))
    advance(factors, tiles, field(u1s), packed_points, g2s, u2s, h_wide, 4, count(1, bs, g1s, u1s))
    advance(factors, tiles, field(u2s), packed_points, g3s, None, h_wide, 4, count(2, bs, g1s, g2s, u2s))
    lane = lane_ids(8)
    pos = place(lane)
    rows = (lane >= GROUP * STEPS) & (lane < GROUP * (STEPS + nx // 2))
    out = jnp.zeros((8, LANES), F32)
    for i, name in enumerate(NAMES):
        p = jnp.where(rows & (pos >= STEPS) & (pos < 2 * STEPS), near.total[name], 0.0)
        q = jnp.where(rows & (pos < STEPS), far.total[name], 0.0)
        s = sums_in[8 * i : 8 * i + 8, :] + (p + q)
        total = jnp.sum(jnp.sum(s, axis=0, keepdims=True), axis=1, keepdims=True)
        out = jnp.where(lane == i, jnp.broadcast_to(total, (8, LANES)), out)
    for i in range(members // 8):
        send[8 * i : 8 * i + 8, :] = out


def fold(v):
    out = v[0:8]
    for i in range(1, v.shape[0] // 8):
        out = out + v[8 * i : 8 * i + 8]
    return out


def solve_small(t):
    g00, g10, g11, g20, g21, g22, m0, m1, m2 = t
    l1, l2 = g10 / g00, g20 / g00
    d1 = g11 - l1 * g10
    e = g21 - l2 * g10
    l3 = e / d1
    d2 = g22 - l2 * g20 - l3 * e
    y1 = m1 - l1 * m0
    y2 = m2 - l2 * m0 - l3 * y1
    c2 = y2 / d2
    c1 = y1 / d1 - l3 * c2
    return m0 / g00 - l1 * c1 - l2 * c2, c1, c2


def combine_kernel(nz, nx, *refs):
    got, b_t, u0, inside_refs, outside_refs = refs[0], refs[1], refs[2], refs[3:8], refs[8:14]
    strips, outs, staged, sems = refs[14:21], refs[21:23], refs[23:25], refs[25]
    g1i, u1i, g2i, u2i, g3i = inside_refs
    u0x, g1x, u1x, g2x, u2x, g3x = outside_refs
    every = range(nx)
    both = lambda level, i, x: Field(nz, (i, inner_rows(nx, level)), (x, outer_rows(nx, level)))
    fields = [Field(nz, (b_t, every)), Field(nz, (u0, every)), both(1, u1i, u1x), both(2, u2i, u2x)]
    fields += [both(1, g1i, g1x), both(2, g2i, g2x), both(3, g3i, g3x)]
    edges_of = [Field(nz, (ref, range(4))) for ref in strips]
    total = jnp.sum(fold(got[...]), axis=0, keepdims=True)
    line = lax.broadcasted_iota(jnp.int32, (1, LANES), 1)
    pick = lambda i: jnp.sum(jnp.where(line == i, total, 0.0), axis=1, keepdims=True)
    c0, c1, c2 = (jnp.broadcast_to(c, (8, LANES)) for c in solve_small([pick(i) for i in range(9)]))
    lane = lane_ids(8)
    inside = (lane >= STEPS) & (lane < LANES - STEPS)
    near_place = place(lane) >= STEPS

    def combined(b, v0, v1, v2, f1, f2, f3):
        return c0 * v0 + c1 * v1 + c2 * v2, b - (c0 * (b - f1) + c1 * (f1 - f2) + c2 * (f2 - f3))

    copies = []
    for block in range(nz // BLOCK):
        for k in range(block * BLOCK, (block + 1) * BLOCK, 8):
            for t in range(2):
                near, far = (combined(*(f.at(j, k) for f in edges_of)) for j in (t, t + 2))
                edges = [jnp.where(near_place, p, q) for p, q in zip(near, far)]
                for u, x, group in strip_places(nx):
                    if u != t or not t * (nx // 2) <= x < (t + 1) * (nx // 2):
                        continue
                    for ref, value, edge in zip(staged, combined(*(f.at(x, k) for f in fields)), edges):
                        turned = pltpu.roll(edge, (-(GROUP * group + STEPS)) % LANES, 1)
                        ref[pl.ds(k * nx + x, 8, stride=nx), :] = jnp.where(inside, value, turned)
        rows = pl.ds(block * BLOCK * nx, BLOCK * nx)
        for i in range(2):
            copies.append(pltpu.make_async_copy(staged[i].at[rows, :], outs[i].at[rows, :], sems.at[i, block]))
            copies[-1].start()
    for copy in copies:
        copy.wait()


def neighbours(array, axes, up):
    size = lax.axis_size(axes)
    pairs = [(i, (i + 1) % size) for i in range(size)]
    return lax.ppermute(array, axes, pairs if up else [(b, a) for a, b in pairs])


def on_device(source_heat, horiz_coef, face_coef, column_inverse):
    nz, nx, ny = source_heat.shape
    gx, gy = "gx", "gy"
    members = lax.axis_size(gx) * lax.axis_size(gy)
    part = lambda f, *a: (lambda *refs: f(*a, *refs))
    nat = source_heat.reshape(nz * nx, ny)
    low, high = pl.pallas_call(
        part(load_kernel, nz, nx),
        in_specs=[spec()],
        out_specs=[spec()] * 2,
        out_shape=[vmem(STEPS * nz)] * 2,
        compiler_params=params(4),
    )(nat)
    below = neighbours(high, gx, True)
    above = neighbours(low, gx, False)
    b_t, u0, h_wide, inner_own, outer_own, *rest = pl.pallas_call(
        part(own_kernel, nz, nx),
        in_specs=[spec()] * 3,
        out_specs=[spec()] * 14,
        out_shape=[vmem(nz * nx), vmem(nz * nx), vmem(nz), vmem(2 * nz), vmem(2 * nz)]
        + [pltpu.VMEM((nz, count * nz), BF16) for count in (3, 2, 1)]
        + [vmem(r * nz) for r in (nx - 2, nx - 2, nx - 4, nx - 4, nx - 6)]
        + [vmem(72)],
        compiler_params=params(8),
        cost_estimate=cost(36 * nz * nz * nx * ny, 1 << 20),
    )(nat, horiz_coef.reshape(1, nz), column_inverse)
    factors, inside, start = rest[:3], rest[3:8], rest[8]
    inner, outer, to_right, to_left = pl.pallas_call(
        part(pack_kernel, nz, nx),
        in_specs=[spec()] * 4,
        out_specs=[spec()] * 4,
        out_shape=[vmem(2 * nz)] * 2 + [vmem(nz)] * 2,
        compiler_params=params(4),
    )(inner_own, outer_own, below, above)
    from_left = neighbours(to_right, gy, True)
    from_right = neighbours(to_left, gy, False)
    *outside, sums = pl.pallas_call(
        part(outer_kernel, nz, nx),
        in_specs=[spec()] * 13,
        out_specs=[spec()] * 7,
        out_shape=[vmem(2 * STEPS * nz)] * 6 + [vmem(72)],
        compiler_params=params(8),
        cost_estimate=cost(36 * nz * nz * 6 * ny, 1 << 20),
    )(b_t, u0, below, above, h_wide, *factors, *inside[:4], start)
    *strips, send = pl.pallas_call(
        part(strip_kernel, nz, nx, members),
        in_specs=[spec()] * 9,
        out_specs=[spec()] * 8,
        out_shape=[vmem(4 * nz)] * 7 + [vmem(members)],
        compiler_params=params(8),
    )(inner, outer, from_left, from_right, h_wide, sums, *factors)
    got = lax.all_to_all(send.reshape(members, 1, LANES), (gx, gy), split_axis=0, concat_axis=0, tiled=True)
    pressure, true_residual = pl.pallas_call(
        part(combine_kernel, nz, nx),
        in_specs=[spec()] * 21,
        out_specs=[pl.BlockSpec(memory_space=pltpu.HBM)] * 2,
        out_shape=[jax.ShapeDtypeStruct((nz * nx, ny), F32)] * 2,
        scratch_shapes=[pltpu.VMEM((nz * nx, ny), F32)] * 2 + [pltpu.SemaphoreType.DMA((2, nz // BLOCK))],
        compiler_params=params(8),
    )(got.reshape(members, LANES), b_t, u0, *inside, *outside, *strips)
    return pressure.reshape(nz, nx, ny), true_residual.reshape(nz, nx, ny)


def solution(mesh):
    field = P(None, "gx", "gy")
    return jax.shard_map(
        on_device,
        mesh=mesh,
        in_specs=(field, P(), P(), P()),
        out_specs=(field, field),
        check_vma=False,
    )
```
